128 devices in a mesh: pp: 2 (over core), ep: 64 (over z, y, x).
Axes of the slice: x: 4, y: 4, z: 4, core: 2. Of those that a mesh axis runs over, the one named last changes fastest.
Arguments:
- x_fwd: bfloat16 [2, 131072, 256], P('pp', 'ep')
- ids_fwd: int32 [2, 131072, 1], P('pp', 'ep')
- gates_fwd: bfloat16 [2, 131072, 1], P('pp', 'ep')
- x_saved: bfloat16 [2, 131072, 256], P('pp', 'ep')
- grad_out: bfloat16 [2, 131072, 256], P('pp', 'ep')
- ids_bwd: int32 [2, 131072, 1], P('pp', 'ep')
- gates_bwd: bfloat16 [2, 131072, 1], P('pp', 'ep')
- w_in: bfloat16 [2, 256, 768], P('pp')
- w_out: bfloat16 [2, 768, 256], P('pp')
- w_gate: bfloat16 [2, 128, 256, 384], P('pp', 'ep')
- w_up: bfloat16 [2, 128, 256, 384], P('pp', 'ep')
- w_down: bfloat16 [2, 128, 384, 256], P('pp', 'ep')
Outputs:
- output 1: bfloat16 [2, 131072, 256], P('pp', 'ep')
- output 2: bfloat16 [2, 131072, 256], P('pp', 'ep')
- output 3: float32 [2, 256, 768], P('pp')
- output 4: float32 [2, 768, 256], P('pp')
- output 5: float32 [2, 128, 256, 384], P('pp', 'ep')
- output 6: float32 [2, 128, 256, 384], P('pp', 'ep')
- output 7: float32 [2, 128, 384, 256], P('pp', 'ep')
All inputs are finite; a program needn't handle non-finite values.
Results may differ from the reference program's by a relative error of at most 0.00833688.
Values are sent between devices in bfloat16 or wider.
A program may use at most 1 GiB of HBM per device.

```python
import jax
import jax.numpy as jnp
from jax import lax

STAGES = 2
EXP_SHARDS = 64
TOK_DEV = 2048
HIDDEN = 256
DENSE_FF = 768
EXPERT_FF = 384
EXPERTS = 128
TOP_K = 1

TOKENS = EXP_SHARDS * TOK_DEV
CAPACITY = 2 * TOK_DEV * TOP_K // EXPERTS
SLOTS = EXP_SHARDS * CAPACITY
EPS = 1e-6


def draw_routes(rng_key):
    avg_load = TOK_DEV * TOP_K // EXPERTS
    levels = jnp.arange(EXPERTS)
    spread = jnp.where(levels < EXPERTS // 4, 2 * avg_load, jnp.where(levels < EXPERTS // 2, avg_load, avg_load // 2))
    positions = jnp.arange(TOK_DEV * TOP_K)

    def one_block(block_key):
        key_a, key_b, key_c = jax.random.split(block_key, 3)
        counts = spread[jax.random.permutation(key_a, EXPERTS)]
        sorted_ids = jnp.searchsorted(jnp.cumsum(counts), positions, side='right')
        id_table = sorted_ids.reshape(TOP_K, TOK_DEV).T
        id_table = id_table[jax.random.permutation(key_b, TOK_DEV)]
        scores = jax.random.randint(key_c, (TOK_DEV, TOP_K), 0, 1024) * TOP_K + jnp.arange(TOP_K)
        return jnp.take_along_axis(id_table, jnp.argsort(scores, axis=1), axis=1)

    routed = jax.vmap(one_block)(jax.random.split(rng_key, EXP_SHARDS))
    return routed.reshape(TOKENS, TOP_K).astype(jnp.int32)


def draw_normal(rng_key, arr_shape, std_dev):
    return (jax.random.normal(rng_key, arr_shape, jnp.float32) * std_dev).astype(jnp.bfloat16)


def setup_inputs(seed: int = 0) -> dict:
    key_list = jax.random.split(jax.random.key(seed), 12)
    tok_shape = (STAGES, TOKENS, HIDDEN)
    route_shape = (STAGES, TOKENS, TOP_K)
    gate_scale = TOP_K ** -0.5
    return {
        'x_fwd': draw_normal(key_list[0], tok_shape, 1.0),
        'ids_fwd': jax.vmap(draw_routes)(jax.random.split(key_list[1], STAGES)),
        'gates_fwd': (jax.random.uniform(key_list[2], route_shape, jnp.float32, 0.5, 1.5) * gate_scale).astype(jnp.bfloat16),
        'x_saved': draw_normal(key_list[3], tok_shape, 1.0),
        'grad_out': draw_normal(key_list[4], tok_shape, 1.0),
        'ids_bwd': jax.vmap(draw_routes)(jax.random.split(key_list[5], STAGES)),
        'gates_bwd': (jax.random.uniform(key_list[6], route_shape, jnp.float32, 0.5, 1.5) * gate_scale).astype(jnp.bfloat16),
        'w_in': draw_normal(key_list[7], (STAGES, HIDDEN, DENSE_FF), HIDDEN ** -0.5),
        'w_out': draw_normal(key_list[8], (STAGES, DENSE_FF, HIDDEN), DENSE_FF ** -0.5),
        'w_gate': draw_normal(key_list[9], (STAGES, EXPERTS, HIDDEN, EXPERT_FF), HIDDEN ** -0.5),
        'w_up': draw_normal(key_list[10], (STAGES, EXPERTS, HIDDEN, EXPERT_FF), HIDDEN ** -0.5),
        'w_down': draw_normal(key_list[11], (STAGES, EXPERTS, EXPERT_FF, HIDDEN), EXPERT_FF ** -0.5),
    }


def rms_norm(x_f32):
    return x_f32 * lax.rsqrt(jnp.mean(x_f32 * x_f32, axis=-1, keepdims=True) + EPS)


def rms_grad(x_f32, grad_in):
    inv_rms = lax.rsqrt(jnp.mean(x_f32 * x_f32, axis=-1, keepdims=True) + EPS)
    return inv_rms * grad_in - x_f32 * inv_rms ** 3 * jnp.mean(grad_in * x_f32, axis=-1, keepdims=True)


def silu_grad(pre_act):
    sig_val = jax.nn.sigmoid(pre_act)
    return sig_val * (1.0 + pre_act * (1.0 - sig_val))


def dense_forward(x_in, w_in, w_out):
    normed = rms_norm(x_in.astype(jnp.float32)).astype(jnp.bfloat16)
    pre_act = jnp.dot(normed, w_in, preferred_element_type=jnp.float32)
    hidden = jax.nn.silu(pre_act).astype(jnp.bfloat16)
    mixed_sum = x_in.astype(jnp.float32) + jnp.dot(hidden, w_out, preferred_element_type=jnp.float32)
    return mixed_sum.astype(jnp.bfloat16), normed, pre_act, hidden


def group_plan(route_ids):
    flat_ids = route_ids.reshape(-1)
    routes = flat_ids.shape[0]
    route_order = jnp.argsort(flat_ids, stable=True)
    counts = jnp.bincount(flat_ids, length=EXPERTS)
    start_pos = jnp.cumsum(counts) - counts
    slot_col = jnp.arange(SLOTS)
    is_valid = slot_col[None, :] < counts[:, None]
    src_route = route_order[jnp.minimum(start_pos[:, None] + slot_col[None, :], routes - 1)]
    slot_rank = jnp.argsort(route_order) - start_pos[flat_ids]
    return src_route, is_valid, flat_ids * SLOTS + slot_rank


def stage_step(stage_args):
    (x_fwd, ids_fwd, gates_fwd, x_saved, grad_out, ids_bwd, gates_bwd, w_in, w_out, w_gate, w_up, w_down) = stage_args
    gate_w = w_gate.astype(jnp.float32)
    up_w = w_up.astype(jnp.float32)
    down_w = w_down.astype(jnp.float32)

    h_fwd = dense_forward(x_fwd, w_in, w_out)[0]
    z_fwd = rms_norm(h_fwd.astype(jnp.float32)).astype(jnp.bfloat16)
    route_f, valid_f, slot_f = group_plan(ids_fwd)
    rows_f = jnp.where(valid_f[..., None], z_fwd[route_f // TOP_K], 0).astype(jnp.float32)
    gate_f = jnp.einsum('emd,edf->emf', rows_f, gate_w)
    up_f = jnp.einsum('emd,edf->emf', rows_f, up_w)
    act_f = (jax.nn.silu(gate_f) * up_f).astype(jnp.bfloat16).astype(jnp.float32)
    out_f = jnp.einsum('emf,efd->emd', act_f, down_w).astype(jnp.bfloat16)
    picked = out_f.reshape(EXPERTS * SLOTS, HIDDEN)[slot_f].reshape(TOKENS, TOP_K, HIDDEN).astype(jnp.float32)
    y_out = (h_fwd.astype(jnp.float32) + jnp.sum(picked * gates_fwd.astype(jnp.float32)[..., None], axis=1)).astype(jnp.bfloat16)

    h_bwd, normed_b, pre_b, hidden_b = dense_forward(x_saved, w_in, w_out)
    z_bwd = rms_norm(h_bwd.astype(jnp.float32)).astype(jnp.bfloat16)
    route_b, valid_b, slot_b = group_plan(ids_bwd)
    tok_b = route_b // TOP_K
    rows_b = jnp.where(valid_b[..., None], z_bwd[tok_b], 0).astype(jnp.float32)
    slot_gate = jnp.where(valid_b, gates_bwd.reshape(-1)[route_b], 0).astype(jnp.float32)
    grad_rows = (grad_out[tok_b].astype(jnp.float32) * slot_gate[..., None]).astype(jnp.bfloat16).astype(jnp.float32)
    gate_b = jnp.einsum('emd,edf->emf', rows_b, gate_w)
    up_b = jnp.einsum('emd,edf->emf', rows_b, up_w)
    gate_act = jax.nn.silu(gate_b)
    act_b = (gate_act * up_b).astype(jnp.bfloat16).astype(jnp.float32)
    dw_down = jnp.einsum('emf,emd->efd', act_b, grad_rows)
    grad_act = jnp.einsum('emd,efd->emf', grad_rows, down_w)
    grad_gate = (grad_act * up_b * silu_grad(gate_b)).astype(jnp.bfloat16).astype(jnp.float32)
    grad_up = (grad_act * gate_act).astype(jnp.bfloat16).astype(jnp.float32)
    dw_gate = jnp.einsum('emd,emf->edf', rows_b, grad_gate)
    dw_up = jnp.einsum('emd,emf->edf', rows_b, grad_up)
    dx_rows = (jnp.einsum('emf,edf->emd', grad_gate, gate_w) + jnp.einsum('emf,edf->emd', grad_up, up_w)).astype(jnp.bfloat16)
    grad_z = jnp.sum(dx_rows.reshape(EXPERTS * SLOTS, HIDDEN)[slot_b].reshape(TOKENS, TOP_K, HIDDEN).astype(jnp.float32), axis=1)
    grad_h = grad_out.astype(jnp.float32) + rms_grad(h_bwd.astype(jnp.float32), grad_z)
    grad_bf = grad_h.astype(jnp.bfloat16)
    grad_hid = jnp.dot(grad_bf, w_out.T, preferred_element_type=jnp.float32)
    grad_pre = (grad_hid * silu_grad(pre_b)).astype(jnp.bfloat16)
    dw_out = jnp.dot(hidden_b.T, grad_bf, preferred_element_type=jnp.float32)
    dw_in = jnp.dot(normed_b.T, grad_pre, preferred_element_type=jnp.float32)
    grad_norm = jnp.dot(grad_pre, w_in.T, preferred_element_type=jnp.float32)
    dx_out = (grad_h + rms_grad(x_saved.astype(jnp.float32), grad_norm)).astype(jnp.bfloat16)
    return y_out, dx_out, dw_in, dw_out, dw_gate, dw_up, dw_down


def reference(x_fwd, ids_fwd, gates_fwd, x_saved, grad_out, ids_bwd, gates_bwd, w_in, w_out, w_gate, w_up, w_down):
    stage_outs = lax.map(stage_step, (x_fwd, ids_fwd, gates_fwd, x_saved, grad_out, ids_bwd, gates_bwd, w_in, w_out, w_gate, w_up, w_down))
    y_out, dx_out, dw_in, dw_out, dw_gate, dw_up, dw_down = stage_outs
    return (jnp.roll(y_out, 1, axis=0), jnp.roll(dx_out, -1, axis=0), dw_in, dw_out, dw_gate, dw_up, dw_down)
```

```python
import functools

import jax
import jax.numpy as jnp
from jax import lax
from jax.experimental import pallas as pl
from jax.experimental.pallas import tpu as pltpu
from jax.sharding import PartitionSpec as P

EPS = 1e-6
F32 = jnp.float32
BF16 = jnp.bfloat16
MIB = 1024 * 1024
ANY = pl.BlockSpec(memory_space=pl.ANY)
VMEM = pl.BlockSpec(memory_space=pltpu.VMEM)


def mm(a, b):
    return lax.dot_general(a, b, (((1,), (0,)), ((), ())), preferred_element_type=F32)


def mm_nt(a, b):
    return lax.dot_general(a, b, (((1,), (1,)), ((), ())), preferred_element_type=F32)


def mm_tn(a, b):
    return lax.dot_general(a, b, (((0,), (0,)), ((), ())), preferred_element_type=F32)


def inv_rms(v):
    return lax.rsqrt(jnp.mean(v * v, axis=-1, keepdims=True) + EPS)


def rms_vjp(v, inv, g):
    return inv * g - v * (inv * inv * inv) * jnp.mean(g * v, axis=-1, keepdims=True)


def plan(ids_ref, slot_ref, n_exp, cap, blk):
    tok = ids_ref.shape[1]
    upper = (lax.broadcasted_iota(jnp.int32, (blk, blk), 0) < lax.broadcasted_iota(jnp.int32, (blk, blk), 1))
    upper = jnp.where(upper, 1.0, 0.0).astype(BF16)
    expert = lax.broadcasted_iota(jnp.int32, (n_exp, blk), 0)
    carry = jnp.zeros((n_exp, 1), F32)
    for b in range(tok // blk):
        ids = ids_ref[:, b * blk:(b + 1) * blk]
        hot = jnp.where(expert == ids, 1.0, 0.0)
        before = mm(hot.astype(BF16), upper) + carry
        rank = jnp.sum(hot * before, axis=0, keepdims=True).astype(jnp.int32)
        carry = carry + jnp.sum(hot, axis=1, keepdims=True)
        slot_ref[:, b * blk:(b + 1) * blk] = (ids & 1) * (n_exp // 2 * cap) + (ids >> 1) * cap + rank


def column(row):
    n = row.shape[1]
    return jnp.transpose(jnp.broadcast_to(row, (128, n)))[:, :1]


def dispatch_chunk(slot_ref, rows_ref, start, size):
    tok = slot_ref.shape[1]
    want = lax.broadcasted_iota(jnp.int32, (size, tok), 0) + start
    pick = jnp.where(want == slot_ref[...], 1.0, 0.0).astype(BF16)
    return mm(pick, rows_ref[...]).astype(BF16)


def combine_chunk(slot_row, back_ref):
    size = slot_row.shape[1]
    slots = back_ref.shape[0]
    lane = lax.broadcasted_iota(jnp.int32, (size, slots), 1)
    pick = jnp.where(lane == column(slot_row), 1.0, 0.0).astype(BF16)
    return mm(pick, back_ref[...])


def dense_tile(x, w_in, w_out):
    inv = inv_rms(x)
    normed = (x * inv).astype(BF16)
    pre = mm(normed, w_in)
    hid = (pre * jax.nn.sigmoid(pre)).astype(BF16)
    h = (x + mm(hid, w_out)).astype(BF16)
    return h


def pre_fwd_kernel(cfg, x_ref, ids_ref, w_in_ref, w_out_ref, send_ref, h_ref, slot_ref, z_ref):
    tok, n_exp, cap, blk, chunk = cfg
    plan(ids_ref, slot_ref, n_exp, cap, blk)

    @pl.loop(0, tok // blk)
    def _(i):
        t = pl.ds(pl.multiple_of(i * blk, blk), blk)
        h = dense_tile(x_ref[t, :].astype(F32), w_in_ref[...], w_out_ref[...])
        h_ref[t, :] = h
        hf = h.astype(F32)
        z_ref[t, :] = (hf * inv_rms(hf)).astype(BF16)

    @pl.loop(0, n_exp * cap // chunk)
    def _(c):
        s = pl.multiple_of(c * chunk, chunk)
        send_ref[pl.ds(s, chunk), :] = dispatch_chunk(slot_ref, z_ref, s, chunk)


def pre_bwd_kernel(cfg, x_ref, g_ref, ids_ref, gate_ref, w_in_ref, w_out_ref, sz_ref, sd_ref, h_ref, slot_ref, zd_ref):
    tok, n_exp, cap, blk, chunk = cfg
    hid = x_ref.shape[1]
    plan(ids_ref, slot_ref, n_exp, cap, blk)

    @pl.loop(0, tok // blk)
    def _(i):
        t = pl.ds(pl.multiple_of(i * blk, blk), blk)
        h = dense_tile(x_ref[t, :].astype(F32), w_in_ref[...], w_out_ref[...])
        h_ref[t, :] = h
        hf = h.astype(F32)
        zd_ref[t, :hid] = (hf * inv_rms(hf)).astype(BF16)
        gate = column(gate_ref[:, t])
        zd_ref[t, hid:] = (gate * g_ref[t, :].astype(F32)).astype(BF16)

    @pl.loop(0, n_exp * cap // chunk)
    def _(c):
        s = pl.multiple_of(c * chunk, chunk)
        both = dispatch_chunk(slot_ref, zd_ref, s, chunk)
        sz_ref[pl.ds(s, chunk), :] = both[:, :hid]
        sd_ref[pl.ds(s, chunk), :] = both[:, hid:]


def expert_fwd_kernel(blk, x_ref, wg_ref, wu_ref, wd_ref, out_ref):
    rows = x_ref.shape[0] // 2
    for e in range(2):
        @pl.loop(0, rows // blk)
        def _(i):
            r = pl.ds(pl.multiple_of(e * rows + i * blk, blk), blk)
            x = x_ref[r, :]
            p = mm(x, wg_ref[e])
            q = mm(x, wu_ref[e])
            act = (p * jax.nn.sigmoid(p) * q).astype(BF16)
            out_ref[r, :] = mm(act, wd_ref[e]).astype(BF16)


def expert_bwd_kernel(blk, x_ref, d_ref, wg_ref, wu_ref, wd_ref, dz_ref, dwg_ref, dwu_ref, dwd_ref, acc_ref):
    rows = x_ref.shape[0] // 2
    for e in range(2):
        dwg_ref[e] = jnp.zeros(dwg_ref.shape[1:], F32)
        dwu_ref[e] = jnp.zeros(dwu_ref.shape[1:], F32)
        acc_ref[...] = jnp.zeros(acc_ref.shape, F32)

        @pl.loop(0, rows // blk)
        def _(i):
            r = pl.ds(pl.multiple_of(e * rows + i * blk, blk), blk)
            x = x_ref[r, :]
            dy = d_ref[r, :]
            p = mm(x, wg_ref[e])
            q = mm(x, wu_ref[e])
            a = mm_nt(dy, wd_ref[e])
            sig = jax.nn.sigmoid(p)
            act_g = p * sig
            act = (act_g * q).astype(BF16)
            dp = (a * q * (sig * (1.0 + p * (1.0 - sig)))).astype(BF16)
            dq = (a * act_g).astype(BF16)
            dz_ref[r, :] = (mm_nt(dp, wg_ref[e]) + mm_nt(dq, wu_ref[e])).astype(BF16)
            dwg_ref[e] += mm_tn(x, dp)
            dwu_ref[e] += mm_tn(x, dq)
            acc_ref[...] += mm_tn(dy, act)

        dwd_ref[e] = jnp.transpose(acc_ref[...])


def post_fwd_kernel(blk, back_ref, slot_ref, gate_ref, h_ref, y_ref):
    @pl.loop(0, h_ref.shape[0] // blk)
    def _(i):
        t = pl.ds(pl.multiple_of(i * blk, blk), blk)
        picked = combine_chunk(slot_ref[:, t], back_ref)
        y_ref[t, :] = (h_ref[t, :].astype(F32) + picked * column(gate_ref[:, t])).astype(BF16)


def post_bwd_kernel(blk, back_ref, slot_ref, h_ref, g_ref, x_ref, w_in_ref, w_out_ref, dx_ref, dwin_ref, dwout_ref, acc_ref):
    dwin_ref[...] = jnp.zeros(dwin_ref.shape, F32)
    acc_ref[...] = jnp.zeros(acc_ref.shape, F32)

    @pl.loop(0, h_ref.shape[0] // blk)
    def _(i):
        t = pl.ds(pl.multiple_of(i * blk, blk), blk)
        gz = combine_chunk(slot_ref[:, t], back_ref)
        h = h_ref[t, :].astype(F32)
        dh = g_ref[t, :].astype(F32) + rms_vjp(h, inv_rms(h), gz)
        b = dh.astype(BF16)
        x = x_ref[t, :].astype(F32)
        inv = inv_rms(x)
        normed = (x * inv).astype(BF16)
        pre = mm(normed, w_in_ref[...])
        sig = jax.nn.sigmoid(pre)
        hid = (pre * sig).astype(BF16)
        da = (mm_nt(b, w_out_ref[...]) * (sig * (1.0 + pre * (1.0 - sig)))).astype(BF16)
        acc_ref[...] += mm_tn(b, hid)
        dwin_ref[...] += mm_tn(normed, da)
        dx_ref[t, :] = (dh + rms_vjp(x, inv, mm_nt(da, w_in_ref[...]))).astype(BF16)

    dwout_ref[...] = jnp.transpose(acc_ref[...])


def vmem_call(kernel, outs, scratch=(), flops=0):
    return pl.pallas_call(
        kernel,
        out_shape=[jax.ShapeDtypeStruct(s, d) for s, d in outs],
        out_specs=[VMEM] * len(outs),
        scratch_shapes=list(scratch),
        compiler_params=pltpu.CompilerParams(vmem_limit_bytes=48 * MIB),
        cost_estimate=pl.CostEstimate(flops=flops, bytes_accessed=8 * MIB, transcendentals=0),
    )


def enter(n_ep):
    me = lax.axis_index('ep')
    barrier = pltpu.get_barrier_semaphore()

    @pl.loop(1, n_ep)
    def _(k):
        pl.semaphore_signal(barrier, inc=1, device_id={'ep': lax.rem(me + k, n_ep)}, device_id_type=pl.DeviceIdType.MESH)

    pl.semaphore_wait(barrier, n_ep - 1)
    return me


def peer(me, k, n_ep):
    side = round(n_ep ** (1 / 3))
    if side ** 3 != n_ep:
        return lax.rem(me + k, n_ep)
    x = lax.rem(lax.rem(me, side) + lax.rem(k, side), side)
    y = lax.rem(me // side % side + k // side % side, side)
    z = lax.rem(me // (side * side) + k // (side * side), side)
    return (z * side + y) * side + x


def exchange_kernel(n_ep, n, *refs):
    ins, outs = refs[:n], refs[n:2 * n]
    send_sem, recv_sem, local_sem = refs[2 * n:]
    me = enter(n_ep)
    for i in range(n):
        pltpu.make_async_copy(ins[i].at[:, me], outs[i].at[:, me], local_sem.at[i]).start()

    @pl.loop(1, n_ep)
    def _(k):
        to = peer(me, k, n_ep)
        for i in range(n):
            pltpu.make_async_remote_copy(
                ins[i].at[:, to], outs[i].at[:, me], send_sem.at[i], recv_sem.at[i],
                device_id={'ep': to}, device_id_type=pl.DeviceIdType.MESH).start()

    for i in range(n):
        pltpu.make_async_copy(ins[i].at[:, me], outs[i].at[:, me], local_sem.at[i]).wait()
        most = pl.ds(0, n_ep - 1)
        pltpu.make_async_copy(ins[i].at[:, most], ins[i].at[:, most], send_sem.at[i]).wait()
        pltpu.make_async_copy(outs[i].at[:, most], outs[i].at[:, most], recv_sem.at[i]).wait()


def exchange(n_ep, cid, *bufs):
    n = len(bufs)
    return pl.pallas_call(
        functools.partial(exchange_kernel, n_ep, n),
        out_shape=[jax.ShapeDtypeStruct(b.shape, b.dtype) for b in bufs],
        in_specs=[ANY] * n,
        out_specs=[ANY] * n,
        scratch_shapes=[pltpu.SemaphoreType.DMA((n,)), pltpu.SemaphoreType.DMA((n,)), pltpu.SemaphoreType.DMA((n,))],
        compiler_params=pltpu.CompilerParams(collective_id=cid, has_side_effects=True),
        cost_estimate=pl.CostEstimate(flops=10 ** 10, bytes_accessed=8 * MIB, transcendentals=0),
    )(*bufs)


def reduce_kernel(n_ep, part_ref, sum_ref):
    total = part_ref[0, 0]
    for i in range(1, n_ep):
        total = total + part_ref[0, i]
    sum_ref[...] = total


def spread_kernel(n_ep, piece_ref, out_ref, send_sem, recv_sem, local_sem):
    me = enter(n_ep)
    own = pltpu.make_async_copy(piece_ref, out_ref.at[me], local_sem)
    own.start()

    @pl.loop(1, n_ep)
    def _(k):
        to = peer(me, k, n_ep)
        pltpu.make_async_remote_copy(
            piece_ref, out_ref.at[me], send_sem, recv_sem,
            device_id={'ep': to}, device_id_type=pl.DeviceIdType.MESH).start()

    own.wait()
    most = out_ref.at[pl.ds(0, n_ep - 1)]
    pltpu.make_async_copy(most, most, send_sem).wait()
    pltpu.make_async_copy(most, most, recv_sem).wait()


def solution(mesh):
    n_ep = mesh.shape['ep']
    n_pp = mesh.shape['pp']
    tok_spec = P('pp', 'ep', None)
    dense_spec = P('pp', None, None)
    exp_spec = P('pp', 'ep', None, None)
    next_perm = [(stage, (stage + 1) % n_pp) for stage in range(n_pp)]
    prev_perm = [(stage, (stage - 1) % n_pp) for stage in range(n_pp)]

    def body(x_fwd, ids_fwd, gates_fwd, x_saved, grad_out, ids_bwd, gates_bwd, w_in, w_out, w_gate, w_up, w_down):
        x_fwd, x_saved, grad_out = x_fwd[0], x_saved[0], grad_out[0]
        w_in, w_out, w_gate, w_up, w_down = w_in[0], w_out[0], w_gate[0], w_up[0], w_down[0]
        tok, hid = x_fwd.shape
        ff = w_in.shape[1]
        n_exp = w_gate.shape[0] * n_ep
        eff = w_gate.shape[2]
        cap = 2 * tok // n_exp
        slots = n_exp * cap
        blk = min(256, tok)
        chunk = min(512, slots)
        cfg = (tok, n_exp, cap, blk, chunk)
        ids_f, ids_b = ids_fwd.reshape(1, tok), ids_bwd.reshape(1, tok)
        gate_f, gate_b = gates_fwd.reshape(1, tok).astype(F32), gates_bwd.reshape(1, tok).astype(F32)
        grouped = (2, n_ep, cap, hid)
        flat = (slots, hid)

        sz, sd, h_b, slot_b = vmem_call(
            functools.partial(pre_bwd_kernel, cfg),
            [(flat, BF16), (flat, BF16), ((tok, hid), BF16), ((1, tok), jnp.int32)],
            [pltpu.VMEM((tok, 2 * hid), BF16)], 11 * 10 ** 9,
        )(x_saved, grad_out, ids_b, gate_b, w_in, w_out)
        rz, rd = exchange(n_ep, 1, sz.reshape(grouped), sd.reshape(grouped))
        sf, h_f, slot_f = vmem_call(
            functools.partial(pre_fwd_kernel, cfg),
            [(flat, BF16), ((tok, hid), BF16), ((1, tok), jnp.int32)],
            [pltpu.VMEM((tok, hid), BF16)], 6 * 10 ** 9,
        )(x_fwd, ids_f, w_in, w_out)
        rf, = exchange(n_ep, 2, sf.reshape(grouped))
        dz, dw_gate, dw_up, dw_down = vmem_call(
            functools.partial(expert_bwd_kernel, blk),
            [(flat, BF16), (w_gate.shape, F32), (w_up.shape, F32), (w_down.shape, F32)],
            [pltpu.VMEM((hid, eff), F32)], 7 * 10 ** 9,
        )(rz.reshape(flat), rd.reshape(flat), w_gate, w_up, w_down)
        bz, = exchange(n_ep, 3, dz.reshape(grouped))
        of, = vmem_call(functools.partial(expert_fwd_kernel, blk), [(flat, BF16)], flops=3 * 10 ** 9)(
            rf.reshape(flat), w_gate, w_up, w_down)
        bf, = exchange(n_ep, 4, of.reshape(grouped))
        dx_out, dw_in, dw_out = vmem_call(
            functools.partial(post_bwd_kernel, blk),
            [((tok, hid), BF16), (w_in.shape, F32), (w_out.shape, F32)],
            [pltpu.VMEM((hid, ff), F32)], 9 * 10 ** 9,
        )(bz.reshape(flat), slot_b, h_b, grad_out, x_saved, w_in, w_out)
        y_out, = vmem_call(functools.partial(post_fwd_kernel, blk), [((tok, hid), BF16)], flops=4 * 10 ** 9)(
            bf.reshape(flat), slot_f, gate_f, h_f)
        y_next = lax.ppermute(y_out, 'pp', next_perm)
        dx_prev = lax.ppermute(dx_out, 'pp', prev_perm)

        lanes = 128
        piece = dw_in.size * 2 // n_ep // lanes
        both = jnp.concatenate([dw_in.reshape(-1, lanes), dw_out.reshape(-1, lanes)], axis=0).reshape(1, n_ep, piece, lanes)
        parts, = exchange(n_ep, 5, both)
        mine, = vmem_call(functools.partial(reduce_kernel, n_ep), [((piece, lanes), F32)])(parts)
        full = pl.pallas_call(
            functools.partial(spread_kernel, n_ep),
            out_shape=jax.ShapeDtypeStruct((n_ep, piece, lanes), F32),
            in_specs=[ANY], out_specs=ANY,
            scratch_shapes=[pltpu.SemaphoreType.DMA] * 3,
            compiler_params=pltpu.CompilerParams(collective_id=6, has_side_effects=True),
        )(mine)
        full = full.reshape(2, -1)
        dw_in, dw_out = full[0].reshape(w_in.shape), full[1].reshape(w_out.shape)
        return (y_next[None], dx_prev[None], dw_in[None], dw_out[None], dw_gate[None], dw_up[None], dw_down[None])

    return jax.shard_map(body, mesh=mesh,
                         in_specs=(tok_spec, tok_spec, tok_spec, tok_spec, tok_spec, tok_spec, tok_spec, dense_spec, dense_spec, exp_spec, exp_spec, exp_spec),
                         out_specs=(tok_spec, tok_spec, dense_spec, dense_spec, exp_spec, exp_spec, exp_spec),
                         check_vma=False)
```

```python
import functools

import jax
import jax.numpy as jnp
from jax import lax
from jax.experimental import pallas as pl
from jax.experimental.pallas import tpu as pltpu
from jax.sharding import PartitionSpec as P

EPS = 1e-6
F32 = jnp.float32
BF16 = jnp.bfloat16
MIB = 1024 * 1024
ANY = pl.BlockSpec(memory_space=pl.ANY)
VMEM = pl.BlockSpec(memory_space=pltpu.VMEM)


def mm(a, b):
    return lax.dot_general(a, b, (((1,), (0,)), ((), ())), preferred_element_type=F32)


def mm_nt(a, b):
    return lax.dot_general(a, b, (((1,), (1,)), ((), ())), preferred_element_type=F32)


def mm_tn(a, b):
    return lax.dot_general(a, b, (((0,), (0,)), ((), ())), preferred_element_type=F32)


def inv_rms(v):
    return lax.rsqrt(jnp.mean(v * v, axis=-1, keepdims=True) + EPS)


def rms_vjp(v, inv, g):
    return inv * g - v * (inv * inv * inv) * jnp.mean(g * v, axis=-1, keepdims=True)


def plan(ids_ref, slot_ref, n_exp, cap, blk):
    tok = ids_ref.shape[1]
    upper = (lax.broadcasted_iota(jnp.int32, (blk, blk), 0) < lax.broadcasted_iota(jnp.int32, (blk, blk), 1))
    upper = jnp.where(upper, 1.0, 0.0).astype(BF16)
    expert = lax.broadcasted_iota(jnp.int32, (n_exp, blk), 0)
    carry = jnp.zeros((n_exp, 1), F32)
    for b in range(tok // blk):
        ids = ids_ref[:, b * blk:(b + 1) * blk]
        hot = jnp.where(expert == ids, 1.0, 0.0)
        before = mm(hot.astype(BF16), upper) + carry
        rank = jnp.sum(hot * before, axis=0, keepdims=True).astype(jnp.int32)
        carry = carry + jnp.sum(hot, axis=1, keepdims=True)
        slot_ref[:, b * blk:(b + 1) * blk] = (ids & 1) * (n_exp // 2 * cap) + (ids >> 1) * cap + rank


def column(row):
    n = row.shape[1]
    return jnp.transpose(jnp.broadcast_to(row, (128, n)))[:, :1]


def dispatch_chunk(slot_ref, rows_ref, start, size):
    tok = slot_ref.shape[1]
    want = lax.broadcasted_iota(jnp.int32, (size, tok), 0) + start
    pick = jnp.where(want == slot_ref[...], 1.0, 0.0).astype(BF16)
    return mm(pick, rows_ref[...]).astype(BF16)


def combine_chunk(slot_row, back_ref):
    size = slot_row.shape[1]
    slots = back_ref.shape[0]
    lane = lax.broadcasted_iota(jnp.int32, (size, slots), 1)
    pick = jnp.where(lane == column(slot_row), 1.0, 0.0).astype(BF16)
    return mm(pick, back_ref[...])


def dense_tile(x, w_in, w_out):
    inv = inv_rms(x)
    normed = (x * inv).astype(BF16)
    pre = mm(normed, w_in)
    hid = (pre * jax.nn.sigmoid(pre)).astype(BF16)
    h = (x + mm(hid, w_out)).astype(BF16)
    return h


def pre_fwd_kernel(cfg, x_ref, ids_ref, w_in_ref, w_out_ref, send_ref, h_ref, slot_ref, z_ref):
    tok, n_exp, cap, blk, chunk = cfg
    plan(ids_ref, slot_ref, n_exp, cap, blk)

    @pl.loop(0, tok // blk)
    def _(i):
        t = pl.ds(pl.multiple_of(i * blk, blk), blk)
        h = dense_tile(x_ref[t, :].astype(F32), w_in_ref[...], w_out_ref[...])
        h_ref[t, :] = h
        hf = h.astype(F32)
        z_ref[t, :] = (hf * inv_rms(hf)).astype(BF16)

    @pl.loop(0, n_exp * cap // chunk)
    def _(c):
        s = pl.multiple_of(c * chunk, chunk)
        send_ref[pl.ds(s, chunk), :] = dispatch_chunk(slot_ref, z_ref, s, chunk)


def pre_bwd_kernel(cfg, x_ref, g_ref, ids_ref, gate_ref, w_in_ref, w_out_ref, sz_ref, sd_ref, h_ref, slot_ref, zd_ref):
    tok, n_exp, cap, blk, chunk = cfg
    hid = x_ref.shape[1]
    plan(ids_ref, slot_ref, n_exp, cap, blk)

    @pl.loop(0, tok // blk)
    def _(i):
        t = pl.ds(pl.multiple_of(i * blk, blk), blk)
        h = dense_tile(x_ref[t, :].astype(F32), w_in_ref[...], w_out_ref[...])
        h_ref[t, :] = h
        hf = h.astype(F32)
        zd_ref[t, :hid] = (hf * inv_rms(hf)).astype(BF16)
        gate = column(gate_ref[:, t])
        zd_ref[t, hid:] = (gate * g_ref[t, :].astype(F32)).astype(BF16)

    @pl.loop(0, n_exp * cap // chunk)
    def _(c):
        s = pl.multiple_of(c * chunk, chunk)
        both = dispatch_chunk(slot_ref, zd_ref, s, chunk)
        sz_ref[pl.ds(s, chunk), :] = both[:, :hid]
        sd_ref[pl.ds(s, chunk), :] = both[:, hid:]


def expert_fwd_kernel(blk, x_ref, wg_ref, wu_ref, wd_ref, out_ref):
    rows = x_ref.shape[0] // 2
    for e in range(2):
        @pl.loop(0, rows // blk)
        def _(i):
            r = pl.ds(pl.multiple_of(e * rows + i * blk, blk), blk)
            x = x_ref[r, :]
            p = mm(x, wg_ref[e])
            q = mm(x, wu_ref[e])
            act = (p * jax.nn.sigmoid(p) * q).astype(BF16)
            out_ref[r, :] = mm(act, wd_ref[e]).astype(BF16)


def expert_bwd_kernel(blk, x_ref, d_ref, wg_ref, wu_ref, wd_ref, dz_ref, dwg_ref, dwu_ref, dwd_ref, acc_ref):
    rows = x_ref.shape[0] // 2
    for e in range(2):
        dwg_ref[e] = jnp.zeros(dwg_ref.shape[1:], F32)
        dwu_ref[e] = jnp.zeros(dwu_ref.shape[1:], F32)
        acc_ref[...] = jnp.zeros(acc_ref.shape, F32)

        @pl.loop(0, rows // blk)
        def _(i):
            r = pl.ds(pl.multiple_of(e * rows + i * blk, blk), blk)
            x = x_ref[r, :]
            dy = d_ref[r, :]
            p = mm(x, wg_ref[e])
            q = mm(x, wu_ref[e])
            a = mm_nt(dy, wd_ref[e])
            sig = jax.nn.sigmoid(p)
            act_g = p * sig
            act = (act_g * q).astype(BF16)
            dp = (a * q * (sig * (1.0 + p * (1.0 - sig)))).astype(BF16)
            dq = (a * act_g).astype(BF16)
            dz_ref[r, :] = (mm_nt(dp, wg_ref[e]) + mm_nt(dq, wu_ref[e])).astype(BF16)
            dwg_ref[e] += mm_tn(x, dp)
            dwu_ref[e] += mm_tn(x, dq)
            acc_ref[...] += mm_tn(dy, act)

        dwd_ref[e] = jnp.transpose(acc_ref[...])


def post_fwd_kernel(blk, back_ref, slot_ref, gate_ref, h_ref, y_ref):
    @pl.loop(0, h_ref.shape[0] // blk)
    def _(i):
        t = pl.ds(pl.multiple_of(i * blk, blk), blk)
        picked = combine_chunk(slot_ref[:, t], back_ref)
        y_ref[t, :] = (h_ref[t, :].astype(F32) + picked * column(gate_ref[:, t])).astype(BF16)


def post_bwd_kernel(blk, back_ref, slot_ref, h_ref, g_ref, x_ref, w_in_ref, w_out_ref, dx_ref, dwin_ref, dwout_ref, acc_ref):
    dwin_ref[...] = jnp.zeros(dwin_ref.shape, F32)
    acc_ref[...] = jnp.zeros(acc_ref.shape, F32)

    @pl.loop(0, h_ref.shape[0] // blk)
    def _(i):
        t = pl.ds(pl.multiple_of(i * blk, blk), blk)
        gz = combine_chunk(slot_ref[:, t], back_ref)
        h = h_ref[t, :].astype(F32)
        dh = g_ref[t, :].astype(F32) + rms_vjp(h, inv_rms(h), gz)
        b = dh.astype(BF16)
        x = x_ref[t, :].astype(F32)
        inv = inv_rms(x)
        normed = (x * inv).astype(BF16)
        pre = mm(normed, w_in_ref[...])
        sig = jax.nn.sigmoid(pre)
        hid = (pre * sig).astype(BF16)
        da = (mm_nt(b, w_out_ref[...]) * (sig * (1.0 + pre * (1.0 - sig)))).astype(BF16)
        acc_ref[...] += mm_tn(b, hid)
        dwin_ref[...] += mm_tn(normed, da)
        dx_ref[t, :] = (dh + rms_vjp(x, inv, mm_nt(da, w_in_ref[...]))).astype(BF16)

    dwout_ref[...] = jnp.transpose(acc_ref[...])


def vmem_call(kernel, outs, scratch=(), flops=0):
    return pl.pallas_call(
        kernel,
        out_shape=[jax.ShapeDtypeStruct(s, d) for s, d in outs],
        out_specs=[VMEM] * len(outs),
        scratch_shapes=list(scratch),
        compiler_params=pltpu.CompilerParams(vmem_limit_bytes=48 * MIB),
        cost_estimate=pl.CostEstimate(flops=flops, bytes_accessed=8 * MIB, transcendentals=0),
    )


def enter(n_ep):
    me = lax.axis_index('ep')
    barrier = pltpu.get_barrier_semaphore()

    @pl.loop(1, n_ep)
    def _(k):
        pl.semaphore_signal(barrier, inc=1, device_id={'ep': lax.rem(me + k, n_ep)}, device_id_type=pl.DeviceIdType.MESH)

    pl.semaphore_wait(barrier, n_ep - 1)
    return me


def peer(me, k, n_ep):
    side = round(n_ep ** (1 / 3))
    if side ** 3 != n_ep:
        return lax.rem(me + k, n_ep)
    x = lax.rem(lax.rem(me, side) + lax.rem(k, side), side)
    y = lax.rem(me // side % side + k // side % side, side)
    z = lax.rem(me // (side * side) + k // (side * side), side)
    return (z * side + y) * side + x


def relays(n_ep):
    if n_ep != 64:
        return [[], [], []]
    rest = [(a, b) for a in (0, 1, 3) for b in (0, 1, 3)][1:]
    offs = [[(2, a, b) for a, b in rest], [(a, 2, b) for a, b in rest], [(a, b, 2) for a, b in rest]]
    return [[x + 4 * y + 16 * z for x, y, z in g] for g in offs]


def exchange_kernel(n_ep, n, side, *refs):
    ins, outs, mid = refs[:n], refs[n:2 * n], refs[2 * n:3 * n]
    send_sem, recv_sem, local_sem, relay_sem, fwd_sem = refs[3 * n:]
    me = enter(n_ep)
    groups = relays(n_ep)
    via = sum(groups, [])
    for i in range(n):
        pltpu.make_async_copy(ins[i].at[:, me], outs[i].at[:, me], local_sem.at[i]).start()

    def send(src, dst, s_sem, r_sem, to):
        pltpu.make_async_remote_copy(src, dst, s_sem, r_sem, device_id={'ep': to}, device_id_type=pl.DeviceIdType.MESH).start()

    for j in range(len(via) // 3):
        for axis, group in enumerate(groups):
            hop = peer(me, side * 4 ** axis, n_ep)
            to = peer(me, group[j], n_ep)
            for i in range(n):
                send(ins[i].at[:, to], mid[i].at[axis, :, j], send_sem.at[i], relay_sem.at[i, axis], hop)
    for k in range(1, n_ep):
        if k in via:
            continue
        to = peer(me, k, n_ep)
        for i in range(n):
            send(ins[i].at[:, to], outs[i].at[:, me], send_sem.at[i], recv_sem.at[i], to)
    if via:
        for i in range(n):
            for axis, group in enumerate(groups):
                pltpu.make_async_copy(mid[i].at[axis], mid[i].at[axis], relay_sem.at[i, axis]).wait()
                origin = peer(me, (4 - side) * 4 ** axis, n_ep)
                for j, k in enumerate(group):
                    send(mid[i].at[axis, :, j], outs[i].at[:, origin], fwd_sem.at[i], recv_sem.at[i], peer(origin, k, n_ep))

    for i in range(n):
        pltpu.make_async_copy(ins[i].at[:, me], outs[i].at[:, me], local_sem.at[i]).wait()
        most = pl.ds(0, n_ep - 1)
        pltpu.make_async_copy(ins[i].at[:, most], ins[i].at[:, most], send_sem.at[i]).wait()
        pltpu.make_async_copy(outs[i].at[:, most], outs[i].at[:, most], recv_sem.at[i]).wait()
        if via:
            pltpu.make_async_copy(mid[i], mid[i], fwd_sem.at[i]).wait()


def exchange(n_ep, cid, *bufs, side=3):
    n = len(bufs)
    rows = max(1, len(relays(n_ep)[0]))
    mids = [jax.ShapeDtypeStruct((3, b.shape[0], rows, *b.shape[2:]), b.dtype) for b in bufs]
    dma = pltpu.SemaphoreType.DMA
    return pl.pallas_call(
        functools.partial(exchange_kernel, n_ep, n, side),
        out_shape=[jax.ShapeDtypeStruct(b.shape, b.dtype) for b in bufs] + mids,
        in_specs=[ANY] * n,
        out_specs=[ANY] * (2 * n),
        scratch_shapes=[dma((n,)), dma((n,)), dma((n,)), dma((n, 3)), dma((n,))],
        compiler_params=pltpu.CompilerParams(collective_id=cid, has_side_effects=True),
        cost_estimate=pl.CostEstimate(flops=10 ** 10, bytes_accessed=8 * MIB, transcendentals=0),
    )(*bufs)[:n]


def reduce_kernel(n_ep, part_ref, sum_ref):
    total = part_ref[0, 0]
    for i in range(1, n_ep):
        total = total + part_ref[0, i]
    sum_ref[...] = total


def spread_kernel(n_ep, piece_ref, out_ref, send_sem, recv_sem, local_sem):
    me = enter(n_ep)
    own = pltpu.make_async_copy(piece_ref, out_ref.at[me], local_sem)
    own.start()

    @pl.loop(1, n_ep)
    def _(k):
        to = peer(me, k, n_ep)
        pltpu.make_async_remote_copy(
            piece_ref, out_ref.at[me], send_sem, recv_sem,
            device_id={'ep': to}, device_id_type=pl.DeviceIdType.MESH).start()

    own.wait()
    most = out_ref.at[pl.ds(0, n_ep - 1)]
    pltpu.make_async_copy(most, most, send_sem).wait()
    pltpu.make_async_copy(most, most, recv_sem).wait()


def solution(mesh):
    n_ep = mesh.shape['ep']
    n_pp = mesh.shape['pp']
    tok_spec = P('pp', 'ep', None)
    dense_spec = P('pp', None, None)
    exp_spec = P('pp', 'ep', None, None)
    next_perm = [(stage, (stage + 1) % n_pp) for stage in range(n_pp)]
    prev_perm = [(stage, (stage - 1) % n_pp) for stage in range(n_pp)]

    def body(x_fwd, ids_fwd, gates_fwd, x_saved, grad_out, ids_bwd, gates_bwd, w_in, w_out, w_gate, w_up, w_down):
        x_fwd, x_saved, grad_out = x_fwd[0], x_saved[0], grad_out[0]
        w_in, w_out, w_gate, w_up, w_down = w_in[0], w_out[0], w_gate[0], w_up[0], w_down[0]
        tok, hid = x_fwd.shape
        ff = w_in.shape[1]
        n_exp = w_gate.shape[0] * n_ep
        eff = w_gate.shape[2]
        cap = 2 * tok // n_exp
        slots = n_exp * cap
        blk = min(256, tok)
        chunk = min(512, slots)
        cfg = (tok, n_exp, cap, blk, chunk)
        ids_f, ids_b = ids_fwd.reshape(1, tok), ids_bwd.reshape(1, tok)
        gate_f, gate_b = gates_fwd.reshape(1, tok).astype(F32), gates_bwd.reshape(1, tok).astype(F32)
        grouped = (2, n_ep, cap, hid)
        flat = (slots, hid)

        sz, sd, h_b, slot_b = vmem_call(
            functools.partial(pre_bwd_kernel, cfg),
            [(flat, BF16), (flat, BF16), ((tok, hid), BF16), ((1, tok), jnp.int32)],
            [pltpu.VMEM((tok, 2 * hid), BF16)], 11 * 10 ** 9,
        )(x_saved, grad_out, ids_b, gate_b, w_in, w_out)
        rz, rd = exchange(n_ep, 1, sz.reshape(grouped), sd.reshape(grouped))
        sf, h_f, slot_f = vmem_call(
            functools.partial(pre_fwd_kernel, cfg),
            [(flat, BF16), ((tok, hid), BF16), ((1, tok), jnp.int32)],
            [pltpu.VMEM((tok, hid), BF16)], 6 * 10 ** 9,
        )(x_fwd, ids_f, w_in, w_out)
        rf, = exchange(n_ep, 2, sf.reshape(grouped), side=1)
        dz, dw_gate, dw_up, dw_down = vmem_call(
            functools.partial(expert_bwd_kernel, blk),
            [(flat, BF16), (w_gate.shape, F32), (w_up.shape, F32), (w_down.shape, F32)],
            [pltpu.VMEM((hid, eff), F32)], 7 * 10 ** 9,
        )(rz.reshape(flat), rd.reshape(flat), w_gate, w_up, w_down)
        bz, = exchange(n_ep, 3, dz.reshape(grouped))
        of, = vmem_call(functools.partial(expert_fwd_kernel, blk), [(flat, BF16)], flops=3 * 10 ** 9)(
            rf.reshape(flat), w_gate, w_up, w_down)
        bf, = exchange(n_ep, 4, of.reshape(grouped))
        dx_out, dw_in, dw_out = vmem_call(
            functools.partial(post_bwd_kernel, blk),
            [((tok, hid), BF16), (w_in.shape, F32), (w_out.shape, F32)],
            [pltpu.VMEM((hid, ff), F32)], 9 * 10 ** 9,
        )(bz.reshape(flat), slot_b, h_b, grad_out, x_saved, w_in, w_out)
        y_out, = vmem_call(functools.partial(post_fwd_kernel, blk), [((tok, hid), BF16)], flops=4 * 10 ** 9)(
            bf.reshape(flat), slot_f, gate_f, h_f)
        y_next = lax.ppermute(y_out, 'pp', next_perm)
        dx_prev = lax.ppermute(dx_out, 'pp', prev_perm)

        lanes = 128
        piece = dw_in.size * 2 // n_ep // lanes
        both = jnp.concatenate([dw_in.reshape(-1, lanes), dw_out.reshape(-1, lanes)], axis=0).reshape(1, n_ep, piece, lanes)
        parts, = exchange(n_ep, 5, both)
        mine, = vmem_call(functools.partial(reduce_kernel, n_ep), [((piece, lanes), F32)])(parts)
        full = pl.pallas_call(
            functools.partial(spread_kernel, n_ep),
            out_shape=jax.ShapeDtypeStruct((n_ep, piece, lanes), F32),
            in_specs=[ANY], out_specs=ANY,
            scratch_shapes=[pltpu.SemaphoreType.DMA] * 3,
            compiler_params=pltpu.CompilerParams(collective_id=6, has_side_effects=True),
        )(mine)
        full = full.reshape(2, -1)
        dw_in, dw_out = full[0].reshape(w_in.shape), full[1].reshape(w_out.shape)
        return (y_next[None], dx_prev[None], dw_in[None], dw_out[None], dw_gate[None], dw_up[None], dw_down[None])

    return jax.shard_map(body, mesh=mesh,
                         in_specs=(tok_spec, tok_spec, tok_spec, tok_spec, tok_spec, tok_spec, tok_spec, dense_spec, dense_spec, exp_spec, exp_spec, exp_spec),
                         out_specs=(tok_spec, tok_spec, dense_spec, dense_spec, exp_spec, exp_spec, exp_spec),
                         check_vma=False)
```

```python
import functools

import jax
import jax.numpy as jnp
from jax import lax
from jax.experimental import pallas as pl
from jax.experimental.pallas import tpu as pltpu
from jax.sharding import PartitionSpec as P

EPS = 1e-6
F32 = jnp.float32
BF16 = jnp.bfloat16
MIB = 1024 * 1024
MESH = pl.DeviceIdType.MESH
ANY = pl.BlockSpec(memory_space=pl.ANY)
VMEM = pl.BlockSpec(memory_space=pltpu.VMEM)


def mm(a, b):
    return lax.dot_general(a, b, (((1,), (0,)), ((), ())), preferred_element_type=F32)


def mm_nt(a, b):
    return lax.dot_general(a, b, (((1,), (1,)), ((), ())), preferred_element_type=F32)


def mm_tn(a, b):
    return lax.dot_general(a, b, (((0,), (0,)), ((), ())), preferred_element_type=F32)


def inv_rms(v):
    return lax.rsqrt(jnp.mean(v * v, axis=-1, keepdims=True) + EPS)


def rms_vjp(v, inv, g):
    return inv * g - v * (inv * inv * inv) * jnp.mean(g * v, axis=-1, keepdims=True)


def plan(ids_ref, slot_ref, n_exp, cap, blk):
    tok = ids_ref.shape[1]
    upper = (lax.broadcasted_iota(jnp.int32, (blk, blk), 0) < lax.broadcasted_iota(jnp.int32, (blk, blk), 1))
    upper = jnp.where(upper, 1.0, 0.0).astype(BF16)
    expert = lax.broadcasted_iota(jnp.int32, (n_exp, blk), 0)
    carry = jnp.zeros((n_exp, 1), F32)
    for b in range(tok // blk):
        ids = ids_ref[:, b * blk:(b + 1) * blk]
        hot = jnp.where(expert == ids, 1.0, 0.0)
        before = mm(hot.astype(BF16), upper) + carry
        rank = jnp.sum(hot * before, axis=0, keepdims=True).astype(jnp.int32)
        carry = carry + jnp.sum(hot, axis=1, keepdims=True)
        slot_ref[:, b * blk:(b + 1) * blk] = (ids & 1) * (n_exp // 2 * cap) + (ids >> 1) * cap + rank


def column(row):
    n = row.shape[1]
    return jnp.transpose(jnp.broadcast_to(row, (128, n)))[:, :1]


def dense_tile(x, w_in, w_out):
    inv = inv_rms(x)
    normed = (x * inv).astype(BF16)
    pre = mm(normed, w_in)
    hid = (pre * jax.nn.sigmoid(pre)).astype(BF16)
    h = (x + mm(hid, w_out)).astype(BF16)
    return h


def dispatch(slot_ref, rows_ref, send_ref, size):
    tok = slot_ref.shape[1]
    half = send_ref.shape[1]
    for j in range(2):
        @pl.loop(0, half // size)
        def _(c):
            start = pl.multiple_of(c * size, size)
            want = lax.broadcasted_iota(jnp.int32, (size, tok), 0) + (start + j * half)
            pick = jnp.where(want == slot_ref[...], 1.0, 0.0).astype(BF16)
            send_ref[j, pl.ds(start, size), :] = mm(pick, rows_ref[...]).astype(BF16)


def combine(slot_row, back_ref):
    size = slot_row.shape[1]
    half = back_ref.shape[1]
    lane = lax.broadcasted_iota(jnp.int32, (size, 2 * half), 1)
    pick = jnp.where(lane == column(slot_row), 1.0, 0.0).astype(BF16)
    return mm(pick, back_ref[...].reshape(2 * half, back_ref.shape[2]))


ORDER = list(range(1, 64))


def step_kernel(cfg, *refs):
    n_pp, n_ep, side, tok, n_exp, cap, blk, chunk, eblk = cfg
    refs = list(refs)

    def take(n):
        got, refs[:] = refs[:n], refs[n:]
        return got

    ids_f, gate_f, ids_b, gate_b = take(4)
    hbm_in = take(8)
    y_out, dx_out, dwin_out, dwout_out, dwg_out, dwu_out, dwd_out = take(7)
    vm_in = take(8)
    grad, x_b, w_in, w_out, x_f, wg, wu, wd = vm_in
    in_sem, = take(1)
    slot_f, slot_b, rows_a, rows_b, h_f, h_b, y, dx = take(8)
    send_d, send_z, send_f, recv_d, recv_z, recv_f = take(6)
    send_dz, send_of, back_dz, back_of = take(4)
    dwg, dwu, dwd, acc_d = take(4)
    part, total, r1, r2, r3, turned = take(6)
    send_sem, recv_sem, local_sem, ar_send, ar_recv, pp_send, pp_recv, out_sem = take(8)

    me = lax.axis_index('ep')
    stage = lax.axis_index('pp')
    coord = [lax.rem(me, side), lax.rem(me // side, side), me // (side * side)]
    weight = [1, side, side * side]

    loads = [pltpu.make_async_copy(a, b, in_sem.at[i]) for i, (a, b) in enumerate(zip(hbm_in, vm_in))]
    for c in loads:
        c.start()

    barrier = pltpu.get_barrier_semaphore()

    @pl.loop(1, n_ep)
    def _(k):
        pl.semaphore_signal(barrier, inc=1, device_id={'ep': lax.rem(me + k, n_ep)}, device_id_type=MESH)

    nxt = lax.rem(stage + 1, n_pp)
    prv = lax.rem(stage + n_pp - 1, n_pp)
    pl.semaphore_signal(barrier, inc=1, device_id={'pp': nxt}, device_id_type=MESH)
    pl.semaphore_signal(barrier, inc=1, device_id={'pp': prv}, device_id_type=MESH)

    def rows_of(dev):
        return pl.ds(pl.multiple_of(dev * cap, cap), cap)

    def peer(k):
        to = 0
        for a in range(3):
            d = k // weight[a] % side
            to = to + weight[a] * lax.rem(coord[a] + lax.rem(stage * (side - d) + (1 - stage) * d, side), side)
        return to

    def start_exchange(x, src, dst):
        pltpu.make_async_copy(src.at[:, rows_of(me)], dst.at[:, rows_of(me)], local_sem.at[x]).start()
        for k in ORDER[:n_ep - 1] if n_ep == 64 else range(1, n_ep):
            to = peer(k)
            pltpu.make_async_remote_copy(
                src.at[:, rows_of(to)], dst.at[:, rows_of(me)], send_sem.at[x], recv_sem.at[x],
                device_id={'ep': to}, device_id_type=MESH).start()

    def most(ref):
        return ref.at[:, pl.ds(0, (n_ep - 1) * cap)]

    def wait_exchange(x, src, dst):
        pltpu.make_async_copy(src.at[:, rows_of(me)], dst.at[:, rows_of(me)], local_sem.at[x]).wait()
        pltpu.make_async_copy(most(dst), most(dst), recv_sem.at[x]).wait()

    def drain_exchange(x, src):
        pltpu.make_async_copy(most(src), most(src), send_sem.at[x]).wait()

    plan(ids_b, slot_b, n_exp, cap, blk)
    loads[0].wait()

    @pl.loop(0, tok // blk)
    def _(i):
        t = pl.ds(pl.multiple_of(i * blk, blk), blk)
        rows_a[t, :] = (column(gate_b[:, t]) * grad[t, :].astype(F32)).astype(BF16)

    dispatch(slot_b, rows_a, send_d, chunk)
    pl.semaphore_wait(barrier, n_ep + 1)
    start_exchange(0, send_d, recv_d)

    for c in loads[1:]:
        c.wait()

    def dense(x_ref, h_ref, z_ref):
        @pl.loop(0, tok // blk)
        def _(i):
            t = pl.ds(pl.multiple_of(i * blk, blk), blk)
            h = dense_tile(x_ref[t, :].astype(F32), w_in[...], w_out[...])
            h_ref[t, :] = h
            hf = h.astype(F32)
            z_ref[t, :] = (hf * inv_rms(hf)).astype(BF16)

    dense(x_b, h_b, rows_b)
    dispatch(slot_b, rows_b, send_z, chunk)
    start_exchange(1, send_z, recv_z)

    plan(ids_f, slot_f, n_exp, cap, blk)
    dense(x_f, h_f, rows_a)
    dispatch(slot_f, rows_a, send_f, chunk)
    start_exchange(2, send_f, recv_f)

    wait_exchange(0, send_d, recv_d)
    wait_exchange(1, send_z, recv_z)
    for e in range(2):
        dwg[e] = jnp.zeros(dwg.shape[1:], F32)
        dwu[e] = jnp.zeros(dwu.shape[1:], F32)
        acc_d[...] = jnp.zeros(acc_d.shape, F32)

        @pl.loop(0, n_ep * cap // eblk)
        def _(i):
            r = pl.ds(pl.multiple_of(i * eblk, eblk), eblk)
            x = recv_z[e, r, :]
            dy = recv_d[e, r, :]
            p = mm(x, wg[e])
            q = mm(x, wu[e])
            a = mm_nt(dy, wd[e])
            sig = jax.nn.sigmoid(p)
            act_g = p * sig
            act = (act_g * q).astype(BF16)
            dp = (a * q * (sig * (1.0 + p * (1.0 - sig)))).astype(BF16)
            dq = (a * act_g).astype(BF16)
            send_dz[e, r, :] = (mm_nt(dp, wg[e]) + mm_nt(dq, wu[e])).astype(BF16)
            dwg[e] += mm_tn(x, dp)
            dwu[e] += mm_tn(x, dq)
            acc_d[...] += mm_tn(dy, act)

        dwd[e] = jnp.transpose(acc_d[...])
    start_exchange(3, send_dz, back_dz)
    early = [pltpu.make_async_copy(a, b, out_sem.at[i]) for i, (a, b) in enumerate(((dwg, dwg_out), (dwu, dwu_out), (dwd, dwd_out)))]
    for c in early:
        c.start()

    wait_exchange(2, send_f, recv_f)
    for e in range(2):
        @pl.loop(0, n_ep * cap // eblk)
        def _(i):
            r = pl.ds(pl.multiple_of(i * eblk, eblk), eblk)
            x = recv_f[e, r, :]
            p = mm(x, wg[e])
            q = mm(x, wu[e])
            act = (p * jax.nn.sigmoid(p) * q).astype(BF16)
            send_of[e, r, :] = mm(act, wd[e]).astype(BF16)
    start_exchange(4, send_of, back_of)

    wait_exchange(3, send_dz, back_dz)
    hid = x_b.shape[1]
    cols = part.shape[2]
    part[...] = jnp.zeros(part.shape, F32)

    @pl.loop(0, tok // blk)
    def _(i):
        t = pl.ds(pl.multiple_of(i * blk, blk), blk)
        gz = combine(slot_b[:, t], back_dz)
        h = h_b[t, :].astype(F32)
        dh = grad[t, :].astype(F32) + rms_vjp(h, inv_rms(h), gz)
        b = dh.astype(BF16)
        x = x_b[t, :].astype(F32)
        inv = inv_rms(x)
        normed = (x * inv).astype(BF16)
        pre = mm(normed, w_in[...])
        sig = jax.nn.sigmoid(pre)
        act = (pre * sig).astype(BF16)
        da = (mm_nt(b, w_out[...]) * (sig * (1.0 + pre * (1.0 - sig)))).astype(BF16)
        dwin = mm_tn(normed, da)
        dwout = mm_tn(b, act)
        for q in range(3):
            part[q, :hid, :] += dwin[:, q * cols:(q + 1) * cols]
            part[q, hid:, :] += dwout[:, q * cols:(q + 1) * cols]
        dx[t, :] = (dh + rms_vjp(x, inv, mm_nt(da, w_in[...]))).astype(BF16)

    def to_stage(ref, out, i, s):
        return pltpu.make_async_remote_copy(ref, out, pp_send.at[i], pp_recv.at[i], device_id={'pp': s}, device_id_type=MESH)

    send_dx = to_stage(dx, dx_out, 0, prv)
    send_dx.start()

    rows = 2 * hid
    size = [rows // side, rows // side ** 2, rows // side ** 3]
    bufs = [r1, r2, r3]

    def base(q, depth):
        at = 0
        for j in range(depth):
            at = at + coord[(q + j) % 3] * size[j]
        return at

    def span(start, n):
        return pl.ds(pl.multiple_of(start, 8), n)

    def along(axis, d):
        c = lax.rem(coord[axis] + d, side)
        return c, me + (c - coord[axis]) * weight[axis]

    def scatter(q, j):
        axis = (q + j) % 3
        for d in range(1, side):
            c, to = along(axis, d)
            pltpu.make_async_remote_copy(
                part.at[q, span(base(q, j) + c * size[j], size[j])], bufs[j].at[q, d - 1],
                ar_send.at[j, q], ar_recv.at[j, q], device_id={'ep': to}, device_id_type=MESH).start()

    def scatter_wait(q, j):
        pltpu.make_async_copy(bufs[j].at[q], bufs[j].at[q], ar_recv.at[j, q]).wait()

    def add(q, j):
        s = span(base(q, j + 1), size[j])
        v = part[q, s, :]
        for d in range(side - 1):
            v = v + bufs[j][q, d]
        if j < 2:
            part[q, s, :] = v
        else:
            total[q, s, :] = v

    def gather(q, j):
        axis = (q + j) % 3
        s = span(base(q, j + 1), size[j])
        for d in range(1, side):
            c, to = along(axis, d)
            pltpu.make_async_remote_copy(
                total.at[q, s], total.at[q, s], ar_send.at[3 + j, q], ar_recv.at[3 + j, q],
                device_id={'ep': to}, device_id_type=MESH).start()

    def gather_wait(q, j):
        n = (side - 1) * size[j]
        pltpu.make_async_copy(total.at[q, pl.ds(0, n)], total.at[q, pl.ds(0, n)], ar_recv.at[3 + j, q]).wait()

    for q in range(3):
        scatter(q, 0)
    for j in range(3):
        for q in range(3):
            scatter_wait(q, j)
            add(q, j)
            if j < 2:
                scatter(q, j + 1)
            else:
                gather(q, 2)
    for j in (2, 1):
        for q in range(3):
            gather_wait(q, j)
            gather(q, j - 1)

    wait_exchange(4, send_of, back_of)

    @pl.loop(0, tok // blk)
    def _(i):
        t = pl.ds(pl.multiple_of(i * blk, blk), blk)
        picked = combine(slot_f[:, t], back_of)
        y[t, :] = (h_f[t, :].astype(F32) + picked * column(gate_f[:, t])).astype(BF16)

    send_y = to_stage(y, y_out, 1, nxt)
    send_y.start()

    late = []
    for q in range(3):
        gather_wait(q, 0)
        late.append(pltpu.make_async_copy(total.at[q, pl.ds(0, hid)], dwin_out.at[:, pl.ds(q * cols, cols)], out_sem.at[3 + q]))
        late[-1].start()
        turned[q * cols:(q + 1) * cols, :] = jnp.transpose(total[q, hid:, :])
    late.append(pltpu.make_async_copy(turned, dwout_out, out_sem.at[6]))
    late[-1].start()

    for x, src in enumerate((send_d, send_z, send_f, send_dz, send_of)):
        drain_exchange(x, src)
    for j in range(3):
        for q in range(3):
            n = pl.ds(0, (side - 1) * size[j])
            pltpu.make_async_copy(total.at[q, n], total.at[q, n], ar_send.at[j, q]).wait()
            pltpu.make_async_copy(total.at[q, n], total.at[q, n], ar_send.at[3 + j, q]).wait()
    for c in early + late:
        c.wait()
    send_dx.wait()
    send_y.wait()


def solution(mesh):
    n_ep = mesh.shape['ep']
    n_pp = mesh.shape['pp']
    side = round(n_ep ** (1 / 3))
    tok_spec = P('pp', 'ep', None)
    dense_spec = P('pp', None, None)
    exp_spec = P('pp', 'ep', None, None)

    def body(x_fwd, ids_fwd, gates_fwd, x_saved, grad_out, ids_bwd, gates_bwd, w_in, w_out, w_gate, w_up, w_down):
        x_fwd, x_saved, grad_out = x_fwd[0], x_saved[0], grad_out[0]
        w_in, w_out, w_gate, w_up, w_down = w_in[0], w_out[0], w_gate[0], w_up[0], w_down[0]
        tok, hid = x_fwd.shape
        ff = w_in.shape[1]
        n_exp = w_gate.shape[0] * n_ep
        eff = w_gate.shape[2]
        cap = 2 * tok // n_exp
        blk = min(256, tok)
        chunk = min(512, n_ep * cap)
        eblk = min(256, n_ep * cap)
        cfg = (n_pp, n_ep, side, tok, n_exp, cap, blk, chunk, eblk)
        ids_f, ids_b = ids_fwd.reshape(1, tok), ids_bwd.reshape(1, tok)
        gate_f, gate_b = gates_fwd.reshape(1, tok).astype(F32), gates_bwd.reshape(1, tok).astype(F32)
        big = [grad_out, x_saved, w_in, w_out, x_fwd, w_gate, w_up, w_down]
        slots = pltpu.VMEM((2, n_ep * cap, hid), BF16)
        rows = pltpu.VMEM((tok, hid), BF16)
        route = pltpu.VMEM((1, tok), jnp.int32)
        dma = pltpu.SemaphoreType.DMA
        cols = ff // 3
        outs = [((tok, hid), BF16)] * 2 + [(w.shape, F32) for w in (w_in, w_out, w_gate, w_up, w_down)]
        y_next, dx_prev, dw_in, dw_out, dw_gate, dw_up, dw_down = pl.pallas_call(
            functools.partial(step_kernel, cfg),
            out_shape=[jax.ShapeDtypeStruct(*o) for o in outs],
            in_specs=[VMEM] * 4 + [ANY] * 8,
            out_specs=[ANY] * 7,
            scratch_shapes=[pltpu.VMEM(b.shape, b.dtype) for b in big] + [dma((8,))]
            + [route] * 2 + [rows] * 6 + [slots] * 10
            + [pltpu.VMEM(w.shape, F32) for w in (w_gate, w_up, w_down)] + [pltpu.VMEM((hid, eff), F32)]
            + [pltpu.VMEM((3, 2 * hid, cols), F32)] * 2
            + [pltpu.VMEM((3, side - 1, 2 * hid // side ** j, cols), F32) for j in (1, 2, 3)]
            + [pltpu.VMEM((ff, hid), F32)]
            + [dma((5,)), dma((5,)), dma((5,)), dma((6, 3)), dma((6, 3)), dma((2,)), dma((2,)), dma((7,))],
            compiler_params=pltpu.CompilerParams(collective_id=0, has_side_effects=True, vmem_limit_bytes=63 * MIB),
        )(ids_f, gate_f, ids_b, gate_b, *big)
        return (y_next[None], dx_prev[None], dw_in[None], dw_out[None], dw_gate[None], dw_up[None], dw_down[None])

    return jax.shard_map(body, mesh=mesh,
                         in_specs=(tok_spec, tok_spec, tok_spec, tok_spec, tok_spec, tok_spec, tok_spec, dense_spec, dense_spec, exp_spec, exp_spec, exp_spec),
                         out_specs=(tok_spec, tok_spec, dense_spec, dense_spec, exp_spec, exp_spec, exp_spec),
                         check_vma=False)
```

```python
import functools

import jax
import jax.numpy as jnp
from jax import lax
from jax.experimental import pallas as pl
from jax.experimental.pallas import tpu as pltpu
from jax.sharding import PartitionSpec as P

EPS = 1e-6
F32 = jnp.float32
BF16 = jnp.bfloat16
MIB = 1024 * 1024
MESH = pl.DeviceIdType.MESH
ANY = pl.BlockSpec(memory_space=pl.ANY)
VMEM = pl.BlockSpec(memory_space=pltpu.VMEM)


def mm(a, b):
    return lax.dot_general(a, b, (((1,), (0,)), ((), ())), preferred_element_type=F32)


def mm_nt(a, b):
    return lax.dot_general(a, b, (((1,), (1,)), ((), ())), preferred_element_type=F32)


def mm_tn(a, b):
    return lax.dot_general(a, b, (((0,), (0,)), ((), ())), preferred_element_type=F32)


def inv_rms(v):
    return lax.rsqrt(jnp.mean(v * v, axis=-1, keepdims=True) + EPS)


def rms_vjp(v, inv, g):
    return inv * g - v * (inv * inv * inv) * jnp.mean(g * v, axis=-1, keepdims=True)


def plan(ids_ref, slot_ref, n_exp, cap, blk):
    tok = ids_ref.shape[1]
    upper = (lax.broadcasted_iota(jnp.int32, (blk, blk), 0) < lax.broadcasted_iota(jnp.int32, (blk, blk), 1))
    upper = jnp.where(upper, 1.0, 0.0).astype(BF16)
    expert = lax.broadcasted_iota(jnp.int32, (n_exp, blk), 0)
    carry = jnp.zeros((n_exp, 1), F32)
    for b in range(tok // blk):
        ids = ids_ref[:, b * blk:(b + 1) * blk]
        hot = jnp.where(expert == ids, 1.0, 0.0)
        before = mm(hot.astype(BF16), upper) + carry
        rank = jnp.sum(hot * before, axis=0, keepdims=True).astype(jnp.int32)
        carry = carry + jnp.sum(hot, axis=1, keepdims=True)
        slot_ref[:, b * blk:(b + 1) * blk] = (ids & 1) * (n_exp // 2 * cap) + (ids >> 1) * cap + rank


def column(row):
    n = row.shape[1]
    return jnp.transpose(jnp.broadcast_to(row, (128, n)))[:, :1]


def dense_tile(x, w_in, w_out):
    inv = inv_rms(x)
    normed = (x * inv).astype(BF16)
    pre = mm(normed, w_in)
    hid = (pre * jax.nn.sigmoid(pre)).astype(BF16)
    h = (x + mm(hid, w_out)).astype(BF16)
    return h


def dispatch(slot_ref, rows_ref, send_ref, j, size):
    tok = slot_ref.shape[1]
    half = send_ref.shape[1]

    @pl.loop(0, half // size)
    def _(c):
        start = pl.multiple_of(c * size, size)
        want = lax.broadcasted_iota(jnp.int32, (size, tok), 0) + (start + j * half)
        pick = jnp.where(want == slot_ref[...], 1.0, 0.0).astype(BF16)
        send_ref[j, pl.ds(start, size), :] = mm(pick, rows_ref[...]).astype(BF16)


def combine(slot_row, back_ref, j):
    size = slot_row.shape[1]
    half = back_ref.shape[1]
    lane = lax.broadcasted_iota(jnp.int32, (size, half), 1) + j * half
    pick = jnp.where(lane == column(slot_row), 1.0, 0.0).astype(BF16)
    return mm(pick, back_ref[j])


ORDER = (
    14, 16, 44, 28, 25, 36, 1, 51, 10, 6, 50, 2, 9, 24, 32, 39, 18, 49, 33, 37, 48,
    12, 60, 41, 40, 8, 61, 13, 29, 62, 22, 59, 7, 20, 21, 63, 31, 45, 5, 26, 34, 47,
    46, 54, 17, 52, 58, 3, 56, 57, 35, 38, 4, 53, 55, 27, 23, 19, 11, 15, 30, 43, 42,
)


def step_kernel(cfg, *refs):
    n_pp, n_ep, side, tok, n_exp, cap, blk, chunk, eblk = cfg
    refs = list(refs)

    def take(n):
        got, refs[:] = refs[:n], refs[n:]
        return got

    ids_f, gate_f, ids_b, gate_b = take(4)
    hbm_in = take(8)
    y_out, dx_out, dwin_out, dwout_out, dwg_out, dwu_out, dwd_out = take(7)
    vm_in = take(8)
    grad, x_b, w_in, w_out, x_f, wg, wu, wd = vm_in
    in_sem, = take(1)
    slot_f, slot_b, rows_a, rows_b, h_f, h_b, y, dx = take(8)
    send_d, send_z, send_f, recv_d, recv_z, recv_f = take(6)
    send_dz, send_of, back_dz, back_of = take(4)
    dwg, dwu, dwd, acc_d = take(4)
    part, total, r1, r2, r3, turned = take(6)
    normed_b, act_b, slope_b, gz_b, gz_f = take(5)
    send_sem, recv_sem, local_sem, ar_send, ar_recv, pp_send, pp_recv, out_sem = take(8)

    me = lax.axis_index('ep')
    stage = lax.axis_index('pp')
    coord = [lax.rem(me, side), lax.rem(me // side, side), me // (side * side)]
    weight = [1, side, side * side]

    loads = [pltpu.make_async_copy(a, b, in_sem.at[i]) for i, (a, b) in enumerate(zip(hbm_in, vm_in))]
    for c in loads:
        c.start()

    barrier = pltpu.get_barrier_semaphore()

    @pl.loop(1, n_ep)
    def _(k):
        pl.semaphore_signal(barrier, inc=1, device_id={'ep': lax.rem(me + k, n_ep)}, device_id_type=MESH)

    nxt = lax.rem(stage + 1, n_pp)
    prv = lax.rem(stage + n_pp - 1, n_pp)
    pl.semaphore_signal(barrier, inc=1, device_id={'pp': nxt}, device_id_type=MESH)
    pl.semaphore_signal(barrier, inc=1, device_id={'pp': prv}, device_id_type=MESH)

    def rows_of(dev):
        return pl.ds(pl.multiple_of(dev * cap, cap), cap)

    def peer(k):
        to = 0
        for a in range(3):
            d = k // weight[a] % side
            to = to + weight[a] * lax.rem(coord[a] + lax.rem(stage * (side - d) + (1 - stage) * d, side), side)
        return to

    order = ORDER if n_ep == 64 else range(1, n_ep)

    def own(x, j, src, dst):
        return pltpu.make_async_copy(src.at[j, rows_of(me)], dst.at[j, rows_of(me)], local_sem.at[x, j])

    def start_exchange(x, j, src, dst, piece=0, pieces=1):
        if piece == 0:
            own(x, j, src, dst).start()
        n = len(order)
        for k in order[n * piece // pieces:n * (piece + 1) // pieces]:
            to = peer(k)
            pltpu.make_async_remote_copy(
                src.at[j, rows_of(to)], dst.at[j, rows_of(me)], send_sem.at[x, j], recv_sem.at[x, j],
                device_id={'ep': to}, device_id_type=MESH).start()

    def most(ref, j):
        return ref.at[j, pl.ds(0, (n_ep - 1) * cap)]

    def wait_exchange(x, j, src, dst):
        own(x, j, src, dst).wait()
        pltpu.make_async_copy(most(dst, j), most(dst, j), recv_sem.at[x, j]).wait()

    def drain_exchange(x, j, src):
        pltpu.make_async_copy(most(src, j), most(src, j), send_sem.at[x, j]).wait()

    plan(ids_b, slot_b, n_exp, cap, blk)
    loads[0].wait()

    @pl.loop(0, tok // blk)
    def _(i):
        t = pl.ds(pl.multiple_of(i * blk, blk), blk)
        rows_a[t, :] = (column(gate_b[:, t].astype(F32)) * grad[t, :].astype(F32)).astype(BF16)

    dispatch(slot_b, rows_a, send_d, 0, chunk)
    pl.semaphore_wait(barrier, n_ep + 1)
    start_exchange(0, 0, send_d, recv_d)

    for c in loads[1:]:
        c.wait()

    @pl.loop(0, tok // blk)
    def _(i):
        t = pl.ds(pl.multiple_of(i * blk, blk), blk)
        x = x_b[t, :].astype(F32)
        normed = (x * inv_rms(x)).astype(BF16)
        pre = mm(normed, w_in[...])
        sig = jax.nn.sigmoid(pre)
        act = (pre * sig).astype(BF16)
        normed_b[t, :] = normed
        act_b[t, :] = act
        slope_b[t, :] = sig * (1.0 + pre * (1.0 - sig))
        h = (x + mm(act, w_out[...])).astype(BF16)
        h_b[t, :] = h
        hf = h.astype(F32)
        rows_b[t, :] = (hf * inv_rms(hf)).astype(BF16)

    dispatch(slot_b, rows_b, send_z, 0, chunk)
    start_exchange(1, 0, send_z, recv_z)
    dispatch(slot_b, rows_a, send_d, 1, chunk)
    start_exchange(0, 1, send_d, recv_d)
    dispatch(slot_b, rows_b, send_z, 1, chunk)
    start_exchange(1, 1, send_z, recv_z)

    plan(ids_f, slot_f, n_exp, cap, blk)

    @pl.loop(0, tok // blk)
    def _(i):
        t = pl.ds(pl.multiple_of(i * blk, blk), blk)
        h = dense_tile(x_f[t, :].astype(F32), w_in[...], w_out[...])
        h_f[t, :] = h
        hf = h.astype(F32)
        rows_a[t, :] = (hf * inv_rms(hf)).astype(BF16)

    for j in range(2):
        dispatch(slot_f, rows_a, send_f, j, chunk)

    def expert_backward(e):
        dwg[e] = jnp.zeros(dwg.shape[1:], F32)
        dwu[e] = jnp.zeros(dwu.shape[1:], F32)
        acc_d[...] = jnp.zeros(acc_d.shape, F32)

        @pl.loop(0, n_ep * cap // eblk)
        def _(i):
            r = pl.ds(pl.multiple_of(i * eblk, eblk), eblk)
            x = recv_z[e, r, :]
            dy = recv_d[e, r, :]
            p = mm(x, wg[e])
            q = mm(x, wu[e])
            a = mm_nt(dy, wd[e])
            sig = jax.nn.sigmoid(p)
            act_g = p * sig
            act = (act_g * q).astype(BF16)
            dp = (a * q * (sig * (1.0 + p * (1.0 - sig)))).astype(BF16)
            dq = (a * act_g).astype(BF16)
            send_dz[e, r, :] = (mm_nt(dp, wg[e]) + mm_nt(dq, wu[e])).astype(BF16)
            dwg[e] += mm_tn(x, dp)
            dwu[e] += mm_tn(x, dq)
            acc_d[...] += mm_tn(dy, act)

        dwd[e] = jnp.transpose(acc_d[...])

    def expert_forward(e):
        @pl.loop(0, n_ep * cap // eblk)
        def _(i):
            r = pl.ds(pl.multiple_of(i * eblk, eblk), eblk)
            x = recv_f[e, r, :]
            p = mm(x, wg[e])
            q = mm(x, wu[e])
            act = (p * jax.nn.sigmoid(p) * q).astype(BF16)
            send_of[e, r, :] = mm(act, wd[e]).astype(BF16)

    for e in range(2):
        wait_exchange(0, e, send_d, recv_d)
        wait_exchange(1, e, send_z, recv_z)
        expert_backward(e)
        start_exchange(3, e, send_dz, back_dz)
    start_exchange(2, 0, send_f, recv_f)
    early = [pltpu.make_async_copy(a, b, out_sem.at[i]) for i, (a, b) in enumerate(((dwg, dwg_out), (dwu, dwu_out), (dwd, dwd_out)))]
    for c in early:
        c.start()

    hid = x_b.shape[1]
    cols = part.shape[2]
    part[...] = jnp.zeros(part.shape, F32)

    def combine_half(x, j, src, back, slot, acc):
        wait_exchange(x, j, src, back)

        @pl.loop(0, tok // blk)
        def _(i):
            t = pl.ds(pl.multiple_of(i * blk, blk), blk)
            acc[t, :] = combine(slot[:, t], back, j)

    combine_half(3, 0, send_dz, back_dz, slot_b, gz_b)
    wait_exchange(3, 1, send_dz, back_dz)

    @pl.loop(0, tok // blk)
    def _(i):
        t = pl.ds(pl.multiple_of(i * blk, blk), blk)
        gz = gz_b[t, :] + combine(slot_b[:, t], back_dz, 1)
        h = h_b[t, :].astype(F32)
        dh = grad[t, :].astype(F32) + rms_vjp(h, inv_rms(h), gz)
        b = dh.astype(BF16)
        da = (mm_nt(b, w_out[...]) * slope_b[t, :]).astype(BF16)
        dwin = mm_tn(normed_b[t, :], da)
        dwout = mm_tn(b, act_b[t, :])
        for q in range(3):
            part[q, :hid, :] += dwin[:, q * cols:(q + 1) * cols]
            part[q, hid:, :] += dwout[:, q * cols:(q + 1) * cols]
        x = x_b[t, :].astype(F32)
        dx[t, :] = (dh + rms_vjp(x, inv_rms(x), mm_nt(da, w_in[...]))).astype(BF16)

    def to_stage(ref, out, i, s):
        return pltpu.make_async_remote_copy(ref, out, pp_send.at[i], pp_recv.at[i], device_id={'pp': s}, device_id_type=MESH)

    send_dx = to_stage(dx, dx_out, 0, prv)
    send_dx.start()

    rows = 2 * hid
    size = [rows // side, rows // side ** 2, rows // side ** 3]
    bufs = [r1, r2, r3]

    def base(q, depth):
        at = 0
        for j in range(depth):
            at = at + coord[(q + j) % 3] * size[j]
        return at

    def span(start, n):
        return pl.ds(pl.multiple_of(start, 8), n)

    def along(axis, d):
        c = lax.rem(coord[axis] + d, side)
        return c, me + (c - coord[axis]) * weight[axis]

    def scatter(q, j):
        axis = (q + j) % 3
        for d in range(1, side):
            c, to = along(axis, d)
            pltpu.make_async_remote_copy(
                part.at[q, span(base(q, j) + c * size[j], size[j])], bufs[j].at[q, d - 1],
                ar_send.at[j, q], ar_recv.at[j, q], device_id={'ep': to}, device_id_type=MESH).start()

    def scatter_wait(q, j):
        pltpu.make_async_copy(bufs[j].at[q], bufs[j].at[q], ar_recv.at[j, q]).wait()

    def add(q, j):
        s = span(base(q, j + 1), size[j])
        v = part[q, s, :]
        for d in range(side - 1):
            v = v + bufs[j][q, d]
        if j < 2:
            part[q, s, :] = v
        else:
            total[q, s, :] = v

    def gather(q, j):
        axis = (q + j) % 3
        s = span(base(q, j + 1), size[j])
        for d in range(1, side):
            c, to = along(axis, d)
            pltpu.make_async_remote_copy(
                total.at[q, s], total.at[q, s], ar_send.at[3 + j, q], ar_recv.at[3 + j, q],
                device_id={'ep': to}, device_id_type=MESH).start()

    def gather_wait(q, j):
        n = (side - 1) * size[j]
        pltpu.make_async_copy(total.at[q, pl.ds(0, n)], total.at[q, pl.ds(0, n)], ar_recv.at[3 + j, q]).wait()

    for q in range(3):
        scatter(q, 0)
    start_exchange(2, 1, send_f, recv_f, 0, 3)
    wait_exchange(2, 0, send_f, recv_f)
    for j in range(3):
        for q in range(3):
            scatter_wait(q, j)
            add(q, j)
            if j < 2:
                scatter(q, j + 1)
            else:
                gather(q, 2)
        if j < 2:
            start_exchange(2, 1, send_f, recv_f, j + 1, 3)
        if j == 0:
            expert_forward(0)
    start_exchange(4, 0, send_of, back_of, 0, 3)
    for j in (2, 1):
        for q in range(3):
            gather_wait(q, j)
            gather(q, j - 1)
        start_exchange(4, 0, send_of, back_of, 3 - j, 3)

    wait_exchange(2, 1, send_f, recv_f)
    expert_forward(1)
    start_exchange(4, 1, send_of, back_of)
    late = []
    for q in range(3):
        gather_wait(q, 0)
        late.append(pltpu.make_async_copy(total.at[q, pl.ds(0, hid)], dwin_out.at[:, pl.ds(q * cols, cols)], out_sem.at[3 + q]))
        late[-1].start()
        turned[q * cols:(q + 1) * cols, :] = jnp.transpose(total[q, hid:, :])
    late.append(pltpu.make_async_copy(turned, dwout_out, out_sem.at[6]))
    late[-1].start()

    combine_half(4, 0, send_of, back_of, slot_f, gz_f)
    wait_exchange(4, 1, send_of, back_of)

    @pl.loop(0, tok // blk)
    def _(i):
        t = pl.ds(pl.multiple_of(i * blk, blk), blk)
        picked = gz_f[t, :] + combine(slot_f[:, t], back_of, 1)
        y[t, :] = (h_f[t, :].astype(F32) + picked * column(gate_f[:, t].astype(F32))).astype(BF16)

    send_y = to_stage(y, y_out, 1, nxt)
    send_y.start()

    for x, src in enumerate((send_d, send_z, send_f, send_dz, send_of)):
        for j in range(2):
            drain_exchange(x, j, src)
    for j in range(3):
        for q in range(3):
            n = pl.ds(0, (side - 1) * size[j])
            pltpu.make_async_copy(total.at[q, n], total.at[q, n], ar_send.at[j, q]).wait()
            pltpu.make_async_copy(total.at[q, n], total.at[q, n], ar_send.at[3 + j, q]).wait()
    for c in early + late:
        c.wait()
    send_dx.wait()
    send_y.wait()


def write_kernel(n, *refs):
    ins, outs, hold, sem = refs[:n], refs[n:2 * n], refs[2 * n:3 * n], refs[3 * n]
    gets = [pltpu.make_async_copy(ins[i], hold[i], sem.at[0, i]) for i in range(n)]
    puts = [pltpu.make_async_copy(hold[i], outs[i], sem.at[1, i]) for i in range(n)]
    for c in gets:
        c.start()
    for get, put in zip(gets, puts):
        get.wait()
        put.start()
    for c in puts:
        c.wait()


def write(*arrays):
    n = len(arrays)
    shapes = [jax.ShapeDtypeStruct(a.shape, a.dtype) for a in arrays]
    return pl.pallas_call(
        functools.partial(write_kernel, n), out_shape=shapes, in_specs=[ANY] * n, out_specs=[ANY] * n,
        scratch_shapes=[pltpu.VMEM(a.shape, a.dtype) for a in arrays] + [pltpu.SemaphoreType.DMA((2, n))],
        compiler_params=pltpu.CompilerParams(vmem_limit_bytes=62 * MIB),
    )(*arrays)


def solution(mesh):
    n_ep = mesh.shape['ep']
    n_pp = mesh.shape['pp']
    side = round(n_ep ** (1 / 3))
    tok_spec = P('pp', 'ep', None)
    dense_spec = P('pp', None, None)
    exp_spec = P('pp', 'ep', None, None)

    def body(x_fwd, ids_fwd, gates_fwd, x_saved, grad_out, ids_bwd, gates_bwd, w_in, w_out, w_gate, w_up, w_down):
        x_fwd, x_saved, grad_out = x_fwd[0], x_saved[0], grad_out[0]
        w_in, w_out, w_gate, w_up, w_down = w_in[0], w_out[0], w_gate[0], w_up[0], w_down[0]
        tok, hid = x_fwd.shape
        ff = w_in.shape[1]
        n_exp = w_gate.shape[0] * n_ep
        eff = w_gate.shape[2]
        cap = 2 * tok // n_exp
        blk = min(256, tok)
        chunk = min(512, n_ep * cap)
        eblk = min(512, n_ep * cap)
        cfg = (n_pp, n_ep, side, tok, n_exp, cap, blk, chunk, eblk)
        ids_f, ids_b = ids_fwd.reshape(1, tok), ids_bwd.reshape(1, tok)
        gate_f, gate_b = gates_fwd.reshape(1, tok), gates_bwd.reshape(1, tok)
        big = [grad_out, x_saved, w_in, w_out, x_fwd, w_gate, w_up, w_down]
        slots = pltpu.VMEM((2, n_ep * cap, hid), BF16)
        rows = pltpu.VMEM((tok, hid), BF16)
        route = pltpu.VMEM((1, tok), jnp.int32)
        dma = pltpu.SemaphoreType.DMA
        cols = ff // 3
        outs = [((tok, hid), BF16)] * 2 + [(w.shape, F32) for w in (w_in, w_out, w_gate, w_up, w_down)]
        results = pl.pallas_call(
            functools.partial(step_kernel, cfg),
            out_shape=[jax.ShapeDtypeStruct(*o) for o in outs],
            in_specs=[VMEM] * 4 + [ANY] * 8,
            out_specs=[ANY] * 7,
            scratch_shapes=[pltpu.VMEM(b.shape, b.dtype) for b in big] + [dma((8,))]
            + [route] * 2 + [rows] * 6 + [slots] * 10
            + [pltpu.VMEM(w.shape, F32) for w in (w_gate, w_up, w_down)] + [pltpu.VMEM((hid, eff), F32)]
            + [pltpu.VMEM((3, 2 * hid, cols), F32)] * 2
            + [pltpu.VMEM((3, side - 1, 2 * hid // side ** j, cols), F32) for j in (1, 2, 3)]
            + [pltpu.VMEM((ff, hid), F32)]
            + [rows, pltpu.VMEM((tok, ff), BF16), pltpu.VMEM((tok, ff), F32), pltpu.VMEM((tok, hid), F32), pltpu.VMEM((tok, hid), F32)]
            + [dma((5, 2)), dma((5, 2)), dma((5, 2)), dma((6, 3)), dma((6, 3)), dma((2,)), dma((2,)), dma((7,))],
            compiler_params=pltpu.CompilerParams(collective_id=0, has_side_effects=True, vmem_limit_bytes=63 * MIB),
        )(ids_f, gate_f, ids_b, gate_b, *big)
        y_next, dx_prev, dw_in, dw_out, dw_gate, dw_up, dw_down = write(*results)
        return (y_next[None], dx_prev[None], dw_in[None], dw_out[None], dw_gate[None], dw_up[None], dw_down[None])

    return jax.shard_map(body, mesh=mesh,
                         in_specs=(tok_spec, tok_spec, tok_spec, tok_spec, tok_spec, tok_spec, tok_spec, dense_spec, dense_spec, exp_spec, exp_spec, exp_spec),
                         out_specs=(tok_spec, tok_spec, dense_spec, dense_spec, exp_spec, exp_spec, exp_spec),
                         check_vma=False)
```

```python
import functools

import jax
import jax.numpy as jnp
from jax import lax
from jax.experimental import pallas as pl
from jax.experimental.pallas import tpu as pltpu
from jax.sharding import PartitionSpec as P

EPS = 1e-6
F32 = jnp.float32
BF16 = jnp.bfloat16
MIB = 1024 * 1024
MESH = pl.DeviceIdType.MESH
ANY = pl.BlockSpec(memory_space=pl.ANY)
VMEM = pl.BlockSpec(memory_space=pltpu.VMEM)


def mm(a, b):
    return lax.dot_general(a, b, (((1,), (0,)), ((), ())), preferred_element_type=F32)


def mm_nt(a, b):
    return lax.dot_general(a, b, (((1,), (1,)), ((), ())), preferred_element_type=F32)


def mm_tn(a, b):
    return lax.dot_general(a, b, (((0,), (0,)), ((), ())), preferred_element_type=F32)


def inv_rms(v):
    return lax.rsqrt(jnp.mean(v * v, axis=-1, keepdims=True) + EPS)


def rms_vjp(v, inv, g):
    return inv * g - v * (inv * inv * inv) * jnp.mean(g * v, axis=-1, keepdims=True)


def plan(ids_ref, slot_ref, n_exp, cap, blk):
    tok = ids_ref.shape[1]
    upper = (lax.broadcasted_iota(jnp.int32, (blk, blk), 0) < lax.broadcasted_iota(jnp.int32, (blk, blk), 1))
    upper = jnp.where(upper, 1.0, 0.0).astype(BF16)
    expert = lax.broadcasted_iota(jnp.int32, (n_exp, blk), 0)
    carry = jnp.zeros((n_exp, 1), F32)
    for b in range(tok // blk):
        ids = ids_ref[:, b * blk:(b + 1) * blk]
        hot = jnp.where(expert == ids, 1.0, 0.0)
        before = mm(hot.astype(BF16), upper) + carry
        rank = jnp.sum(hot * before, axis=0, keepdims=True).astype(jnp.int32)
        carry = carry + jnp.sum(hot, axis=1, keepdims=True)
        slot_ref[:, b * blk:(b + 1) * blk] = (ids & 1) * (n_exp // 2 * cap) + (ids >> 1) * cap + rank


def column(row):
    n = row.shape[1]
    return jnp.transpose(jnp.broadcast_to(row, (128, n)))[:, :1]


def dense_tile(x, w_in, w_out):
    inv = inv_rms(x)
    normed = (x * inv).astype(BF16)
    pre = mm(normed, w_in)
    hid = (pre * jax.nn.sigmoid(pre)).astype(BF16)
    h = (x + mm(hid, w_out)).astype(BF16)
    return h


def dispatch(slot_ref, rows_ref, send_ref, j, size):
    tok = slot_ref.shape[1]
    half = send_ref.shape[1]

    @pl.loop(0, half // size)
    def _(c):
        start = pl.multiple_of(c * size, size)
        want = lax.broadcasted_iota(jnp.int32, (size, tok), 0) + (start + j * half)
        pick = jnp.where(want == slot_ref[...], 1.0, 0.0).astype(BF16)
        send_ref[j, pl.ds(start, size), :] = mm(pick, rows_ref[...]).astype(BF16)


def combine(slot_row, back_ref, j):
    size = slot_row.shape[1]
    half = back_ref.shape[1]
    lane = lax.broadcasted_iota(jnp.int32, (size, half), 1) + j * half
    pick = jnp.where(lane == column(slot_row), 1.0, 0.0).astype(BF16)
    return mm(pick, back_ref[j])


ORDER = (
    14, 16, 44, 28, 25, 36, 1, 51, 10, 6, 50, 2, 9, 24, 32, 39, 18, 49, 33, 37, 48,
    12, 60, 41, 40, 8, 61, 13, 29, 62, 22, 59, 7, 20, 21, 63, 31, 45, 5, 26, 34, 47,
    46, 54, 17, 52, 58, 3, 56, 57, 35, 38, 4, 53, 55, 27, 23, 19, 11, 15, 30, 43, 42,
)


def step_kernel(cfg, *refs):
    n_pp, n_ep, side, tok, n_exp, cap, blk, chunk, eblk = cfg
    refs = list(refs)

    def take(n):
        got, refs[:] = refs[:n], refs[n:]
        return got

    ids_f, gate_f, ids_b, gate_b = take(4)
    hbm_in = take(8)
    y_out, dx_out, dwin_out, dwout_out, dwg_out, dwu_out, dwd_out = take(7)
    vm_in = take(8)
    grad, x_b, w_in, w_out, x_f, wg, wu, wd = vm_in
    in_sem, = take(1)
    slot_f, slot_b, rows_a, rows_b, h_f, h_b, y, dx = take(8)
    send_d, send_z, send_f, recv_d, recv_z, recv_f = take(6)
    send_dz, send_of, back_dz, back_of = take(4)
    dwg, dwu, dwd, acc_d = take(4)
    part, total, r1, r2, r3, turned = take(6)
    normed_b, act_b, slope_b, gz_b, gz_f = take(5)
    send_sem, recv_sem, local_sem, ar_send, ar_recv, pp_send, pp_recv, out_sem = take(8)

    me = lax.axis_index('ep')
    stage = lax.axis_index('pp')
    coord = [lax.rem(me, side), lax.rem(me // side, side), me // (side * side)]
    weight = [1, side, side * side]

    loads = [pltpu.make_async_copy(a, b, in_sem.at[i]) for i, (a, b) in enumerate(zip(hbm_in, vm_in))]
    for c in loads:
        c.start()

    barrier = pltpu.get_barrier_semaphore()

    @pl.loop(1, n_ep)
    def _(k):
        pl.semaphore_signal(barrier, inc=1, device_id={'ep': lax.rem(me + k, n_ep)}, device_id_type=MESH)

    nxt = lax.rem(stage + 1, n_pp)
    prv = lax.rem(stage + n_pp - 1, n_pp)
    pl.semaphore_signal(barrier, inc=1, device_id={'pp': nxt}, device_id_type=MESH)
    pl.semaphore_signal(barrier, inc=1, device_id={'pp': prv}, device_id_type=MESH)

    def rows_of(dev):
        return pl.ds(pl.multiple_of(dev * cap, cap), cap)

    def peer(k):
        to = 0
        for a in range(3):
            d = k // weight[a] % side
            to = to + weight[a] * lax.rem(coord[a] + lax.rem(stage * (side - d) + (1 - stage) * d, side), side)
        return to

    order = ORDER if n_ep == 64 else range(1, n_ep)

    def own(x, j, src, dst):
        return pltpu.make_async_copy(src.at[j, rows_of(me)], dst.at[j, rows_of(me)], local_sem.at[x, j])

    def start_exchange(x, j, src, dst, piece=0, pieces=1):
        if piece == 0:
            own(x, j, src, dst).start()
        n = len(order)
        for k in order[n * piece // pieces:n * (piece + 1) // pieces]:
            to = peer(k)
            pltpu.make_async_remote_copy(
                src.at[j, rows_of(to)], dst.at[j, rows_of(me)], send_sem.at[x, j], recv_sem.at[x, j],
                device_id={'ep': to}, device_id_type=MESH).start()

    def most(ref, j):
        return ref.at[j, pl.ds(0, (n_ep - 1) * cap)]

    def wait_exchange(x, j, src, dst):
        own(x, j, src, dst).wait()
        pltpu.make_async_copy(most(dst, j), most(dst, j), recv_sem.at[x, j]).wait()

    def drain_exchange(x, j, src):
        pltpu.make_async_copy(most(src, j), most(src, j), send_sem.at[x, j]).wait()

    plan(ids_b, slot_b, n_exp, cap, blk)
    loads[0].wait()

    @pl.loop(0, tok // blk)
    def _(i):
        t = pl.ds(pl.multiple_of(i * blk, blk), blk)
        rows_a[t, :] = (column(gate_b[:, t].astype(F32)) * grad[t, :].astype(F32)).astype(BF16)

    dispatch(slot_b, rows_a, send_d, 0, chunk)
    pl.semaphore_wait(barrier, n_ep + 1)
    start_exchange(0, 0, send_d, recv_d)

    for c in loads[1:]:
        c.wait()

    @pl.loop(0, tok // blk)
    def _(i):
        t = pl.ds(pl.multiple_of(i * blk, blk), blk)
        x = x_b[t, :].astype(F32)
        normed = (x * inv_rms(x)).astype(BF16)
        pre = mm(normed, w_in[...])
        sig = jax.nn.sigmoid(pre)
        act = (pre * sig).astype(BF16)
        normed_b[t, :] = normed
        act_b[t, :] = act
        slope_b[t, :] = sig * (1.0 + pre * (1.0 - sig))
        h = (x + mm(act, w_out[...])).astype(BF16)
        h_b[t, :] = h
        hf = h.astype(F32)
        rows_b[t, :] = (hf * inv_rms(hf)).astype(BF16)

    dispatch(slot_b, rows_b, send_z, 0, chunk)
    start_exchange(1, 0, send_z, recv_z)
    dispatch(slot_b, rows_a, send_d, 1, chunk)
    start_exchange(0, 1, send_d, recv_d)
    dispatch(slot_b, rows_b, send_z, 1, chunk)
    start_exchange(1, 1, send_z, recv_z)

    plan(ids_f, slot_f, n_exp, cap, blk)

    @pl.loop(0, tok // blk)
    def _(i):
        t = pl.ds(pl.multiple_of(i * blk, blk), blk)
        h = dense_tile(x_f[t, :].astype(F32), w_in[...], w_out[...])
        h_f[t, :] = h
        hf = h.astype(F32)
        rows_a[t, :] = (hf * inv_rms(hf)).astype(BF16)

    for j in range(2):
        dispatch(slot_f, rows_a, send_f, j, chunk)

    def expert_backward(e):
        dwg[e] = jnp.zeros(dwg.shape[1:], F32)
        dwu[e] = jnp.zeros(dwu.shape[1:], F32)
        acc_d[...] = jnp.zeros(acc_d.shape, F32)

        @pl.loop(0, n_ep * cap // eblk)
        def _(i):
            r = pl.ds(pl.multiple_of(i * eblk, eblk), eblk)
            x = recv_z[e, r, :]
            dy = recv_d[e, r, :]
            p = mm(x, wg[e])
            q = mm(x, wu[e])
            a = mm_nt(dy, wd[e])
            sig = jax.nn.sigmoid(p)
            act_g = p * sig
            act = (act_g * q).astype(BF16)
            dp = (a * q * (sig * (1.0 + p * (1.0 - sig)))).astype(BF16)
            dq = (a * act_g).astype(BF16)
            send_dz[e, r, :] = (mm_nt(dp, wg[e]) + mm_nt(dq, wu[e])).astype(BF16)
            dwg[e] += mm_tn(x, dp)
            dwu[e] += mm_tn(x, dq)
            acc_d[...] += mm_tn(dy, act)

        dwd[e] = jnp.transpose(acc_d[...])

    def expert_forward(e):
        @pl.loop(0, n_ep * cap // eblk)
        def _(i):
            r = pl.ds(pl.multiple_of(i * eblk, eblk), eblk)
            x = recv_f[e, r, :]
            p = mm(x, wg[e])
            q = mm(x, wu[e])
            act = (p * jax.nn.sigmoid(p) * q).astype(BF16)
            send_of[e, r, :] = mm(act, wd[e]).astype(BF16)

    for e in range(2):
        wait_exchange(0, e, send_d, recv_d)
        wait_exchange(1, e, send_z, recv_z)
        expert_backward(e)
        start_exchange(3, e, send_dz, back_dz)
    for e in range(2):
        start_exchange(2, e, send_f, recv_f)
    early = [pltpu.make_async_copy(a, b, out_sem.at[i]) for i, (a, b) in enumerate(((dwg, dwg_out), (dwu, dwu_out), (dwd, dwd_out)))]
    for c in early:
        c.start()

    hid = x_b.shape[1]
    cols = part.shape[2]
    part[...] = jnp.zeros(part.shape, F32)

    def combine_half(x, j, src, back, slot, acc):
        wait_exchange(x, j, src, back)

        @pl.loop(0, tok // blk)
        def _(i):
            t = pl.ds(pl.multiple_of(i * blk, blk), blk)
            acc[t, :] = combine(slot[:, t], back, j)

    combine_half(3, 0, send_dz, back_dz, slot_b, gz_b)
    wait_exchange(3, 1, send_dz, back_dz)

    @pl.loop(0, tok // blk)
    def _(i):
        t = pl.ds(pl.multiple_of(i * blk, blk), blk)
        gz = gz_b[t, :] + combine(slot_b[:, t], back_dz, 1)
        h = h_b[t, :].astype(F32)
        dh = grad[t, :].astype(F32) + rms_vjp(h, inv_rms(h), gz)
        b = dh.astype(BF16)
        da = (mm_nt(b, w_out[...]) * slope_b[t, :]).astype(BF16)
        dwin = mm_tn(normed_b[t, :], da)
        dwout = mm_tn(b, act_b[t, :])
        for q in range(3):
            part[q, :hid, :] += dwin[:, q * cols:(q + 1) * cols]
            part[q, hid:, :] += dwout[:, q * cols:(q + 1) * cols]
        x = x_b[t, :].astype(F32)
        dx[t, :] = (dh + rms_vjp(x, inv_rms(x), mm_nt(da, w_in[...]))).astype(BF16)

    def to_stage(ref, out, i, s):
        return pltpu.make_async_remote_copy(ref, out, pp_send.at[i], pp_recv.at[i], device_id={'pp': s}, device_id_type=MESH)

    send_dx = to_stage(dx, dx_out, 0, prv)
    send_dx.start()

    rows = 2 * hid
    size = [rows // side, rows // side ** 2, rows // side ** 3]
    bufs = [r1, r2, r3]

    def base(q, depth):
        at = 0
        for j in range(depth):
            at = at + coord[(q + j) % 3] * size[j]
        return at

    def span(start, n):
        return pl.ds(pl.multiple_of(start, 8), n)

    def along(axis, d):
        c = lax.rem(coord[axis] + d, side)
        return c, me + (c - coord[axis]) * weight[axis]

    def scatter(q, j):
        axis = (q + j) % 3
        for d in range(1, side):
            c, to = along(axis, d)
            pltpu.make_async_remote_copy(
                part.at[q, span(base(q, j) + c * size[j], size[j])], bufs[j].at[q, d - 1],
                ar_send.at[j, q], ar_recv.at[j, q], device_id={'ep': to}, device_id_type=MESH).start()

    def scatter_wait(q, j):
        pltpu.make_async_copy(bufs[j].at[q], bufs[j].at[q], ar_recv.at[j, q]).wait()

    def add(q, j):
        s = span(base(q, j + 1), size[j])
        v = part[q, s, :]
        for d in range(side - 1):
            v = v + bufs[j][q, d]
        if j < 2:
            part[q, s, :] = v
        else:
            total[q, s, :] = v

    def gather(q, j):
        axis = (q + j) % 3
        s = span(base(q, j + 1), size[j])
        for d in range(1, side):
            c, to = along(axis, d)
            pltpu.make_async_remote_copy(
                total.at[q, s], total.at[q, s], ar_send.at[3 + j, q], ar_recv.at[3 + j, q],
                device_id={'ep': to}, device_id_type=MESH).start()

    def gather_wait(q, j):
        n = (side - 1) * size[j]
        pltpu.make_async_copy(total.at[q, pl.ds(0, n)], total.at[q, pl.ds(0, n)], ar_recv.at[3 + j, q]).wait()

    for q in range(3):
        scatter(q, 0)
    wait_exchange(2, 0, send_f, recv_f)
    expert_forward(0)
    start_exchange(4, 0, send_of, back_of, 0, 2)
    wait_exchange(2, 1, send_f, recv_f)
    expert_forward(1)
    for j in range(3):
        for q in range(3):
            scatter_wait(q, j)
            add(q, j)
            if j < 2:
                scatter(q, j + 1)
            else:
                gather(q, 2)
        start_exchange(4, (j + 1) // 2, send_of, back_of, (j + 1) % 2, 2)
    for j in (2, 1):
        for q in range(3):
            gather_wait(q, j)
            gather(q, j - 1)

    combine_half(4, 0, send_of, back_of, slot_f, gz_f)
    wait_exchange(4, 1, send_of, back_of)

    @pl.loop(0, tok // blk)
    def _(i):
        t = pl.ds(pl.multiple_of(i * blk, blk), blk)
        picked = gz_f[t, :] + combine(slot_f[:, t], back_of, 1)
        y[t, :] = (h_f[t, :].astype(F32) + picked * column(gate_f[:, t].astype(F32))).astype(BF16)

    send_y = to_stage(y, y_out, 1, nxt)
    send_y.start()

    late = []
    for q in range(3):
        gather_wait(q, 0)
        late.append(pltpu.make_async_copy(total.at[q, pl.ds(0, hid)], dwin_out.at[:, pl.ds(q * cols, cols)], out_sem.at[3 + q]))
        late[-1].start()
        turned[q * cols:(q + 1) * cols, :] = jnp.transpose(total[q, hid:, :])
    late.append(pltpu.make_async_copy(turned, dwout_out, out_sem.at[6]))
    late[-1].start()

    for x, src in enumerate((send_d, send_z, send_f, send_dz, send_of)):
        for j in range(2):
            drain_exchange(x, j, src)
    for j in range(3):
        for q in range(3):
            n = pl.ds(0, (side - 1) * size[j])
            pltpu.make_async_copy(total.at[q, n], total.at[q, n], ar_send.at[j, q]).wait()
            pltpu.make_async_copy(total.at[q, n], total.at[q, n], ar_send.at[3 + j, q]).wait()
    for c in early + late:
        c.wait()
    send_dx.wait()
    send_y.wait()


def write_kernel(n, *refs):
    ins, outs, hold, sem = refs[:n], refs[n:2 * n], refs[2 * n:3 * n], refs[3 * n]
    gets = [pltpu.make_async_copy(ins[i], hold[i], sem.at[0, i]) for i in range(n)]
    puts = [pltpu.make_async_copy(hold[i], outs[i], sem.at[1, i]) for i in range(n)]
    for c in gets:
        c.start()
    for get, put in zip(gets, puts):
        get.wait()
        put.start()
    for c in puts:
        c.wait()


def write(*arrays):
    n = len(arrays)
    shapes = [jax.ShapeDtypeStruct(a.shape, a.dtype) for a in arrays]
    return pl.pallas_call(
        functools.partial(write_kernel, n), out_shape=shapes, in_specs=[ANY] * n, out_specs=[ANY] * n,
        scratch_shapes=[pltpu.VMEM(a.shape, a.dtype) for a in arrays] + [pltpu.SemaphoreType.DMA((2, n))],
        compiler_params=pltpu.CompilerParams(vmem_limit_bytes=62 * MIB),
    )(*arrays)


def solution(mesh):
    n_ep = mesh.shape['ep']
    n_pp = mesh.shape['pp']
    side = round(n_ep ** (1 / 3))
    tok_spec = P('pp', 'ep', None)
    dense_spec = P('pp', None, None)
    exp_spec = P('pp', 'ep', None, None)

    def body(x_fwd, ids_fwd, gates_fwd, x_saved, grad_out, ids_bwd, gates_bwd, w_in, w_out, w_gate, w_up, w_down):
        x_fwd, x_saved, grad_out = x_fwd[0], x_saved[0], grad_out[0]
        w_in, w_out, w_gate, w_up, w_down = w_in[0], w_out[0], w_gate[0], w_up[0], w_down[0]
        tok, hid = x_fwd.shape
        ff = w_in.shape[1]
        n_exp = w_gate.shape[0] * n_ep
        eff = w_gate.shape[2]
        cap = 2 * tok // n_exp
        blk = min(256, tok)
        chunk = min(512, n_ep * cap)
        eblk = min(512, n_ep * cap)
        cfg = (n_pp, n_ep, side, tok, n_exp, cap, blk, chunk, eblk)
        ids_f, ids_b = ids_fwd.reshape(1, tok), ids_bwd.reshape(1, tok)
        gate_f, gate_b = gates_fwd.reshape(1, tok), gates_bwd.reshape(1, tok)
        big = [grad_out, x_saved, w_in, w_out, x_fwd, w_gate, w_up, w_down]
        slots = pltpu.VMEM((2, n_ep * cap, hid), BF16)
        rows = pltpu.VMEM((tok, hid), BF16)
        route = pltpu.VMEM((1, tok), jnp.int32)
        dma = pltpu.SemaphoreType.DMA
        cols = ff // 3
        outs = [((tok, hid), BF16)] * 2 + [(w.shape, F32) for w in (w_in, w_out, w_gate, w_up, w_down)]
        results = pl.pallas_call(
            functools.partial(step_kernel, cfg),
            out_shape=[jax.ShapeDtypeStruct(*o) for o in outs],
            in_specs=[VMEM] * 4 + [ANY] * 8,
            out_specs=[ANY] * 7,
            scratch_shapes=[pltpu.VMEM(b.shape, b.dtype) for b in big] + [dma((8,))]
            + [route] * 2 + [rows] * 6 + [slots] * 10
            + [pltpu.VMEM(w.shape, F32) for w in (w_gate, w_up, w_down)] + [pltpu.VMEM((hid, eff), F32)]
            + [pltpu.VMEM((3, 2 * hid, cols), F32)] * 2
            + [pltpu.VMEM((3, side - 1, 2 * hid // side ** j, cols), F32) for j in (1, 2, 3)]
            + [pltpu.VMEM((ff, hid), F32)]
            + [rows, pltpu.VMEM((tok, ff), BF16), pltpu.VMEM((tok, ff), F32), pltpu.VMEM((tok, hid), F32), pltpu.VMEM((tok, hid), F32)]
            + [dma((5, 2)), dma((5, 2)), dma((5, 2)), dma((6, 3)), dma((6, 3)), dma((2,)), dma((2,)), dma((7,))],
            compiler_params=pltpu.CompilerParams(collective_id=0, has_side_effects=True, vmem_limit_bytes=63 * MIB),
        )(ids_f, gate_f, ids_b, gate_b, *big)
        y_next, dx_prev, dw_in, dw_out, dw_gate, dw_up, dw_down = write(*results)
        return (y_next[None], dx_prev[None], dw_in[None], dw_out[None], dw_gate[None], dw_up[None], dw_down[None])

    return jax.shard_map(body, mesh=mesh,
                         in_specs=(tok_spec, tok_spec, tok_spec, tok_spec, tok_spec, tok_spec, tok_spec, dense_spec, dense_spec, exp_spec, exp_spec, exp_spec),
                         out_specs=(tok_spec, tok_spec, dense_spec, dense_spec, exp_spec, exp_spec, exp_spec),
                         check_vma=False)
```

```python
import functools

import jax
import jax.numpy as jnp
from jax import lax
from jax.experimental import pallas as pl
from jax.experimental.pallas import tpu as pltpu
from jax.sharding import PartitionSpec as P

EPS = 1e-6
F32 = jnp.float32
BF16 = jnp.bfloat16
MIB = 1024 * 1024
MESH = pl.DeviceIdType.MESH
ANY = pl.BlockSpec(memory_space=pl.ANY)
VMEM = pl.BlockSpec(memory_space=pltpu.VMEM)


def mm(a, b):
    return lax.dot_general(a, b, (((1,), (0,)), ((), ())), preferred_element_type=F32)


def mm_nt(a, b):
    return lax.dot_general(a, b, (((1,), (1,)), ((), ())), preferred_element_type=F32)


def mm_tn(a, b):
    return lax.dot_general(a, b, (((0,), (0,)), ((), ())), preferred_element_type=F32)


def inv_rms(v):
    return lax.rsqrt(jnp.mean(v * v, axis=-1, keepdims=True) + EPS)


def rms_vjp(v, inv, g):
    return inv * g - v * (inv * inv * inv) * jnp.mean(g * v, axis=-1, keepdims=True)


def plan(ids_ref, slot_ref, n_exp, cap, blk):
    tok = ids_ref.shape[1]
    upper = (lax.broadcasted_iota(jnp.int32, (blk, blk), 0) < lax.broadcasted_iota(jnp.int32, (blk, blk), 1))
    upper = jnp.where(upper, 1.0, 0.0).astype(BF16)
    expert = lax.broadcasted_iota(jnp.int32, (n_exp, blk), 0)
    carry = jnp.zeros((n_exp, 1), F32)
    for b in range(tok // blk):
        ids = ids_ref[:, b * blk:(b + 1) * blk]
        hot = jnp.where(expert == ids, 1.0, 0.0)
        before = mm(hot.astype(BF16), upper) + carry
        rank = jnp.sum(hot * before, axis=0, keepdims=True).astype(jnp.int32)
        carry = carry + jnp.sum(hot, axis=1, keepdims=True)
        slot_ref[:, b * blk:(b + 1) * blk] = (ids & 1) * (n_exp // 2 * cap) + (ids >> 1) * cap + rank


def column(row):
    n = row.shape[1]
    return jnp.transpose(jnp.broadcast_to(row, (128, n)))[:, :1]


def dense_tile(x, w_in, w_out):
    inv = inv_rms(x)
    normed = (x * inv).astype(BF16)
    pre = mm(normed, w_in)
    hid = (pre * jax.nn.sigmoid(pre)).astype(BF16)
    h = (x + mm(hid, w_out)).astype(BF16)
    return h


def dispatch(slot_ref, rows_ref, send_ref, j, size):
    tok = slot_ref.shape[1]
    half = send_ref.shape[1]

    @pl.loop(0, half // size)
    def _(c):
        start = pl.multiple_of(c * size, size)
        want = lax.broadcasted_iota(jnp.int32, (size, tok), 0) + (start + j * half)
        pick = jnp.where(want == slot_ref[...], 1.0, 0.0).astype(BF16)
        send_ref[j, pl.ds(start, size), :] = mm(pick, rows_ref[...]).astype(BF16)


def combine(slot_row, back_ref, j):
    size = slot_row.shape[1]
    half = back_ref.shape[1]
    lane = lax.broadcasted_iota(jnp.int32, (size, half), 1) + j * half
    pick = jnp.where(lane == column(slot_row), 1.0, 0.0).astype(BF16)
    return mm(pick, back_ref[j])


ORDER = (
    14, 16, 44, 28, 25, 36, 1, 51, 10, 6, 50, 2, 9, 24, 32, 39, 18, 49, 33, 37, 48,
    12, 60, 41, 40, 8, 61, 13, 29, 62, 22, 59, 7, 20, 21, 63, 31, 45, 5, 26, 34, 47,
    46, 54, 17, 52, 58, 3, 56, 57, 35, 38, 4, 53, 55, 27, 23, 19, 11, 15, 30, 43, 42,
)


def step_kernel(cfg, *refs):
    n_pp, n_ep, side, tok, n_exp, cap, blk, chunk, eblk = cfg
    refs = list(refs)

    def take(n):
        got, refs[:] = refs[:n], refs[n:]
        return got

    ids_f, gate_f, ids_b, gate_b = take(4)
    hbm_in = take(8)
    y_out, dx_out, dwin_out, dwout_out, dwg_out, dwu_out, dwd_out = take(7)
    vm_in = take(8)
    grad, x_b, w_in, w_out, x_f, wg, wu, wd = vm_in
    in_sem, = take(1)
    slot_f, slot_b, rows_a, rows_b, h_f, h_b, y, dx = take(8)
    send_d, send_z, send_f, recv_d, recv_z, recv_f = take(6)
    send_dz, send_of, back_dz, back_of = take(4)
    dwg, dwu, dwd, acc_d = take(4)
    part, total, r1, r2, turned = take(5)
    normed_b, act_b, slope_b, gz_b, gz_f = take(5)
    send_sem, recv_sem, local_sem, ar_send, ar_recv, pp_send, pp_recv, out_sem = take(8)

    me = lax.axis_index('ep')
    stage = lax.axis_index('pp')
    coord = [lax.rem(me, side), lax.rem(me // side, side), me // (side * side)]
    weight = [1, side, side * side]

    loads = [pltpu.make_async_copy(a, b, in_sem.at[i]) for i, (a, b) in enumerate(zip(hbm_in, vm_in))]
    for c in loads:
        c.start()

    barrier = pltpu.get_barrier_semaphore()

    @pl.loop(1, n_ep)
    def _(k):
        pl.semaphore_signal(barrier, inc=1, device_id={'ep': lax.rem(me + k, n_ep)}, device_id_type=MESH)

    nxt = lax.rem(stage + 1, n_pp)
    prv = lax.rem(stage + n_pp - 1, n_pp)
    pl.semaphore_signal(barrier, inc=1, device_id={'pp': nxt}, device_id_type=MESH)
    pl.semaphore_signal(barrier, inc=1, device_id={'pp': prv}, device_id_type=MESH)

    def rows_of(dev):
        return pl.ds(pl.multiple_of(dev * cap, cap), cap)

    def peer(k):
        to = 0
        for a in range(3):
            d = k // weight[a] % side
            to = to + weight[a] * lax.rem(coord[a] + lax.rem(stage * (side - d) + (1 - stage) * d, side), side)
        return to

    order = ORDER if n_ep == 64 else range(1, n_ep)

    def own(x, j, src, dst):
        return pltpu.make_async_copy(src.at[j, rows_of(me)], dst.at[j, rows_of(me)], local_sem.at[x, j])

    def start_exchange(x, j, src, dst, piece=0, pieces=1):
        if piece == 0:
            own(x, j, src, dst).start()
        n = len(order)
        for k in order[n * piece // pieces:n * (piece + 1) // pieces]:
            to = peer(k)
            pltpu.make_async_remote_copy(
                src.at[j, rows_of(to)], dst.at[j, rows_of(me)], send_sem.at[x, j], recv_sem.at[x, j],
                device_id={'ep': to}, device_id_type=MESH).start()

    def most(ref, j):
        return ref.at[j, pl.ds(0, (n_ep - 1) * cap)]

    def wait_exchange(x, j, src, dst):
        own(x, j, src, dst).wait()
        pltpu.make_async_copy(most(dst, j), most(dst, j), recv_sem.at[x, j]).wait()

    def drain_exchange(x, j, src):
        pltpu.make_async_copy(most(src, j), most(src, j), send_sem.at[x, j]).wait()

    plan(ids_b, slot_b, n_exp, cap, blk)
    loads[0].wait()

    @pl.loop(0, tok // blk)
    def _(i):
        t = pl.ds(pl.multiple_of(i * blk, blk), blk)
        rows_a[t, :] = (column(gate_b[:, t].astype(F32)) * grad[t, :].astype(F32)).astype(BF16)

    dispatch(slot_b, rows_a, send_d, 0, chunk)
    pl.semaphore_wait(barrier, n_ep + 1)
    start_exchange(0, 0, send_d, recv_d)

    for c in loads[1:]:
        c.wait()

    @pl.loop(0, tok // blk)
    def _(i):
        t = pl.ds(pl.multiple_of(i * blk, blk), blk)
        x = x_b[t, :].astype(F32)
        normed = (x * inv_rms(x)).astype(BF16)
        pre = mm(normed, w_in[...])
        sig = jax.nn.sigmoid(pre)
        act = (pre * sig).astype(BF16)
        normed_b[t, :] = normed
        act_b[t, :] = act
        slope_b[t, :] = sig * (1.0 + pre * (1.0 - sig))
        h = (x + mm(act, w_out[...])).astype(BF16)
        h_b[t, :] = h
        hf = h.astype(F32)
        rows_b[t, :] = (hf * inv_rms(hf)).astype(BF16)

    dispatch(slot_b, rows_b, send_z, 0, chunk)
    start_exchange(1, 0, send_z, recv_z)
    dispatch(slot_b, rows_a, send_d, 1, chunk)
    start_exchange(0, 1, send_d, recv_d)
    dispatch(slot_b, rows_b, send_z, 1, chunk)
    start_exchange(1, 1, send_z, recv_z)

    plan(ids_f, slot_f, n_exp, cap, blk)

    @pl.loop(0, tok // blk)
    def _(i):
        t = pl.ds(pl.multiple_of(i * blk, blk), blk)
        h = dense_tile(x_f[t, :].astype(F32), w_in[...], w_out[...])
        h_f[t, :] = h
        hf = h.astype(F32)
        rows_a[t, :] = (hf * inv_rms(hf)).astype(BF16)

    for j in range(2):
        dispatch(slot_f, rows_a, send_f, j, chunk)

    def expert_backward(e):
        dwg[e] = jnp.zeros(dwg.shape[1:], F32)
        dwu[e] = jnp.zeros(dwu.shape[1:], F32)
        acc_d[...] = jnp.zeros(acc_d.shape, F32)

        @pl.loop(0, n_ep * cap // eblk)
        def _(i):
            r = pl.ds(pl.multiple_of(i * eblk, eblk), eblk)
            x = recv_z[e, r, :]
            dy = recv_d[e, r, :]
            p = mm(x, wg[e])
            q = mm(x, wu[e])
            a = mm_nt(dy, wd[e])
            sig = jax.nn.sigmoid(p)
            act_g = p * sig
            act = (act_g * q).astype(BF16)
            dp = (a * q * (sig * (1.0 + p * (1.0 - sig)))).astype(BF16)
            dq = (a * act_g).astype(BF16)
            send_dz[e, r, :] = (mm_nt(dp, wg[e]) + mm_nt(dq, wu[e])).astype(BF16)
            dwg[e] += mm_tn(x, dp)
            dwu[e] += mm_tn(x, dq)
            acc_d[...] += mm_tn(dy, act)

        dwd[e] = jnp.transpose(acc_d[...])

    def expert_forward(e):
        @pl.loop(0, n_ep * cap // eblk)
        def _(i):
            r = pl.ds(pl.multiple_of(i * eblk, eblk), eblk)
            x = recv_f[e, r, :]
            p = mm(x, wg[e])
            q = mm(x, wu[e])
            act = (p * jax.nn.sigmoid(p) * q).astype(BF16)
            send_of[e, r, :] = mm(act, wd[e]).astype(BF16)

    for e in range(2):
        wait_exchange(0, e, send_d, recv_d)
        wait_exchange(1, e, send_z, recv_z)
        expert_backward(e)
        start_exchange(3, e, send_dz, back_dz)
    start_exchange(2, 0, send_f, recv_f)
    start_exchange(2, 1, send_f, recv_f, 0, 2)
    early = [pltpu.make_async_copy(a, b, out_sem.at[i]) for i, (a, b) in enumerate(((dwg, dwg_out), (dwu, dwu_out), (dwd, dwd_out)))]
    for c in early:
        c.start()

    hid = x_b.shape[1]
    cols = part.shape[2]
    part[...] = jnp.zeros(part.shape, F32)

    def combine_half(x, j, src, back, slot, acc):
        wait_exchange(x, j, src, back)

        @pl.loop(0, tok // blk)
        def _(i):
            t = pl.ds(pl.multiple_of(i * blk, blk), blk)
            acc[t, :] = combine(slot[:, t], back, j)

    combine_half(3, 0, send_dz, back_dz, slot_b, gz_b)
    wait_exchange(3, 1, send_dz, back_dz)

    @pl.loop(0, tok // blk)
    def _(i):
        t = pl.ds(pl.multiple_of(i * blk, blk), blk)
        gz = gz_b[t, :] + combine(slot_b[:, t], back_dz, 1)
        h = h_b[t, :].astype(F32)
        dh = grad[t, :].astype(F32) + rms_vjp(h, inv_rms(h), gz)
        b = dh.astype(BF16)
        da = (mm_nt(b, w_out[...]) * slope_b[t, :]).astype(BF16)
        dwin = mm_tn(normed_b[t, :], da)
        dwout = mm_tn(b, act_b[t, :])
        for q in range(3):
            part[q, :hid, :] += dwin[:, q * cols:(q + 1) * cols]
            part[q, hid:, :] += dwout[:, q * cols:(q + 1) * cols]
        x = x_b[t, :].astype(F32)
        dx[t, :] = (dh + rms_vjp(x, inv_rms(x), mm_nt(da, w_in[...]))).astype(BF16)

    def to_stage(ref, out, i, s):
        return pltpu.make_async_remote_copy(ref, out, pp_send.at[i], pp_recv.at[i], device_id={'pp': s}, device_id_type=MESH)

    send_dx = to_stage(dx, dx_out, 0, prv)
    send_dx.start()

    rows = 2 * hid
    wide, narrow = rows // side, rows // side ** 3
    plane = [(b, c) for b in range(side) for c in range(side)][1:]

    def span(start, n):
        return pl.ds(pl.multiple_of(start, 8), n)

    def row_of(q, b, c):
        return coord[q] * wide + (b * side + c) * narrow

    def shifted(axis, d):
        return lax.rem(coord[axis] + d, side)

    def push(src, dst, phase, q, to):
        pltpu.make_async_remote_copy(src, dst, ar_send.at[phase, q], ar_recv.at[phase, q], device_id={'ep': to}, device_id_type=MESH).start()

    def plane_peers(q):
        b0, c0 = (q + 1) % 3, (q + 2) % 3
        for i, (db, dc) in enumerate(plane):
            b, c = shifted(b0, db), shifted(c0, dc)
            yield i, b, c, me + (b - coord[b0]) * weight[b0] + (c - coord[c0]) * weight[c0]

    def mine(q):
        return span(row_of(q, coord[(q + 1) % 3], coord[(q + 2) % 3]), narrow)

    def scatter_axis(q):
        for d in range(1, side):
            c = shifted(q, d)
            push(part.at[q, span(c * wide, wide)], r1.at[q, d - 1], 0, q, me + (c - coord[q]) * weight[q])

    def scatter_plane(q):
        pltpu.make_async_copy(r1.at[q], r1.at[q], ar_recv.at[0, q]).wait()
        s = span(coord[q] * wide, wide)
        v = part[q, s, :]
        for d in range(side - 1):
            v = v + r1[q, d]
        part[q, s, :] = v
        for i, b, c, to in plane_peers(q):
            push(part.at[q, span(row_of(q, b, c), narrow)], r2.at[q, i], 1, q, to)

    def gather_plane(q):
        pltpu.make_async_copy(r2.at[q], r2.at[q], ar_recv.at[1, q]).wait()
        v = part[q, mine(q), :]
        for i in range(len(plane)):
            v = v + r2[q, i]
        total[q, mine(q), :] = v
        for i, b, c, to in plane_peers(q):
            push(total.at[q, mine(q)], total.at[q, mine(q)], 2, q, to)

    def gather_axis(q):
        n = pl.ds(0, len(plane) * narrow)
        pltpu.make_async_copy(total.at[q, n], total.at[q, n], ar_recv.at[2, q]).wait()
        s = span(coord[q] * wide, wide)
        for d in range(1, side):
            c = shifted(q, d)
            push(total.at[q, s], total.at[q, s], 3, q, me + (c - coord[q]) * weight[q])

    def gathered(q):
        n = pl.ds(0, (side - 1) * wide)
        pltpu.make_async_copy(total.at[q, n], total.at[q, n], ar_recv.at[3, q]).wait()

    for q in range(3):
        scatter_axis(q)
    start_exchange(2, 1, send_f, recv_f, 1, 2)
    wait_exchange(2, 0, send_f, recv_f)
    expert_forward(0)
    for q in range(3):
        scatter_plane(q)
    start_exchange(4, 0, send_of, back_of, 0, 2)
    wait_exchange(2, 1, send_f, recv_f)
    expert_forward(1)
    for q in range(3):
        gather_plane(q)
    start_exchange(4, 0, send_of, back_of, 1, 2)
    start_exchange(4, 1, send_of, back_of, 0, 2)
    for q in range(3):
        gather_axis(q)
    start_exchange(4, 1, send_of, back_of, 1, 2)

    combine_half(4, 0, send_of, back_of, slot_f, gz_f)
    wait_exchange(4, 1, send_of, back_of)

    @pl.loop(0, tok // blk)
    def _(i):
        t = pl.ds(pl.multiple_of(i * blk, blk), blk)
        picked = gz_f[t, :] + combine(slot_f[:, t], back_of, 1)
        y[t, :] = (h_f[t, :].astype(F32) + picked * column(gate_f[:, t].astype(F32))).astype(BF16)

    send_y = to_stage(y, y_out, 1, nxt)
    send_y.start()

    late = []
    for q in range(3):
        gathered(q)
        late.append(pltpu.make_async_copy(total.at[q, pl.ds(0, hid)], dwin_out.at[:, pl.ds(q * cols, cols)], out_sem.at[3 + q]))
        late[-1].start()
        turned[q * cols:(q + 1) * cols, :] = jnp.transpose(total[q, hid:, :])
    late.append(pltpu.make_async_copy(turned, dwout_out, out_sem.at[6]))
    late[-1].start()

    for x, src in enumerate((send_d, send_z, send_f, send_dz, send_of)):
        for j in range(2):
            drain_exchange(x, j, src)
    for q in range(3):
        for phase, n in enumerate(((side - 1) * wide, len(plane) * narrow, len(plane) * narrow, (side - 1) * wide)):
            pltpu.make_async_copy(total.at[q, pl.ds(0, n)], total.at[q, pl.ds(0, n)], ar_send.at[phase, q]).wait()
    for c in early + late:
        c.wait()
    send_dx.wait()
    send_y.wait()


def write_kernel(n, *refs):
    ins, outs, hold, sem = refs[:n], refs[n:2 * n], refs[2 * n:3 * n], refs[3 * n]
    gets = [pltpu.make_async_copy(ins[i], hold[i], sem.at[0, i]) for i in range(n)]
    puts = [pltpu.make_async_copy(hold[i], outs[i], sem.at[1, i]) for i in range(n)]
    for c in gets:
        c.start()
    for get, put in zip(gets, puts):
        get.wait()
        put.start()
    for c in puts:
        c.wait()


def write(*arrays):
    n = len(arrays)
    shapes = [jax.ShapeDtypeStruct(a.shape, a.dtype) for a in arrays]
    return pl.pallas_call(
        functools.partial(write_kernel, n), out_shape=shapes, in_specs=[ANY] * n, out_specs=[ANY] * n,
        scratch_shapes=[pltpu.VMEM(a.shape, a.dtype) for a in arrays] + [pltpu.SemaphoreType.DMA((2, n))],
        compiler_params=pltpu.CompilerParams(vmem_limit_bytes=62 * MIB),
    )(*arrays)


def solution(mesh):
    n_ep = mesh.shape['ep']
    n_pp = mesh.shape['pp']
    side = round(n_ep ** (1 / 3))
    tok_spec = P('pp', 'ep', None)
    dense_spec = P('pp', None, None)
    exp_spec = P('pp', 'ep', None, None)

    def body(x_fwd, ids_fwd, gates_fwd, x_saved, grad_out, ids_bwd, gates_bwd, w_in, w_out, w_gate, w_up, w_down):
        x_fwd, x_saved, grad_out = x_fwd[0], x_saved[0], grad_out[0]
        w_in, w_out, w_gate, w_up, w_down = w_in[0], w_out[0], w_gate[0], w_up[0], w_down[0]
        tok, hid = x_fwd.shape
        ff = w_in.shape[1]
        n_exp = w_gate.shape[0] * n_ep
        eff = w_gate.shape[2]
        cap = 2 * tok // n_exp
        blk = min(256, tok)
        chunk = min(512, n_ep * cap)
        eblk = min(512, n_ep * cap)
        cfg = (n_pp, n_ep, side, tok, n_exp, cap, blk, chunk, eblk)
        ids_f, ids_b = ids_fwd.reshape(1, tok), ids_bwd.reshape(1, tok)
        gate_f, gate_b = gates_fwd.reshape(1, tok), gates_bwd.reshape(1, tok)
        big = [grad_out, x_saved, w_in, w_out, x_fwd, w_gate, w_up, w_down]
        slots = pltpu.VMEM((2, n_ep * cap, hid), BF16)
        rows = pltpu.VMEM((tok, hid), BF16)
        route = pltpu.VMEM((1, tok), jnp.int32)
        dma = pltpu.SemaphoreType.DMA
        cols = ff // 3
        outs = [((tok, hid), BF16)] * 2 + [(w.shape, F32) for w in (w_in, w_out, w_gate, w_up, w_down)]
        results = pl.pallas_call(
            functools.partial(step_kernel, cfg),
            out_shape=[jax.ShapeDtypeStruct(*o) for o in outs],
            in_specs=[VMEM] * 4 + [ANY] * 8,
            out_specs=[ANY] * 7,
            scratch_shapes=[pltpu.VMEM(b.shape, b.dtype) for b in big] + [dma((8,))]
            + [route] * 2 + [rows] * 6 + [slots] * 10
            + [pltpu.VMEM(w.shape, F32) for w in (w_gate, w_up, w_down)] + [pltpu.VMEM((hid, eff), F32)]
            + [pltpu.VMEM((3, 2 * hid, cols), F32)] * 2
            + [pltpu.VMEM((3, side ** j - 1, 2 * hid // side ** (2 * j - 1), cols), F32) for j in (1, 2)]
            + [pltpu.VMEM((ff, hid), F32)]
            + [rows, pltpu.VMEM((tok, ff), BF16), pltpu.VMEM((tok, ff), F32), pltpu.VMEM((tok, hid), F32), pltpu.VMEM((tok, hid), F32)]
            + [dma((5, 2)), dma((5, 2)), dma((5, 2)), dma((4, 3)), dma((4, 3)), dma((2,)), dma((2,)), dma((7,))],
            compiler_params=pltpu.CompilerParams(collective_id=0, has_side_effects=True, vmem_limit_bytes=63 * MIB),
        )(ids_f, gate_f, ids_b, gate_b, *big)
        y_next, dx_prev, dw_in, dw_out, dw_gate, dw_up, dw_down = write(*results)
        return (y_next[None], dx_prev[None], dw_in[None], dw_out[None], dw_gate[None], dw_up[None], dw_down[None])

    return jax.shard_map(body, mesh=mesh,
                         in_specs=(tok_spec, tok_spec, tok_spec, tok_spec, tok_spec, tok_spec, tok_spec, dense_spec, dense_spec, exp_spec, exp_spec, exp_spec),
                         out_specs=(tok_spec, tok_spec, dense_spec, dense_spec, exp_spec, exp_spec, exp_spec),
                         check_vma=False)
```

```python
import functools

import jax
import jax.numpy as jnp
from jax import lax
from jax.experimental import pallas as pl
from jax.experimental.pallas import tpu as pltpu
from jax.sharding import PartitionSpec as P

EPS = 1e-6
F32 = jnp.float32
BF16 = jnp.bfloat16
MIB = 1024 * 1024
MESH = pl.DeviceIdType.MESH
ANY = pl.BlockSpec(memory_space=pl.ANY)
VMEM = pl.BlockSpec(memory_space=pltpu.VMEM)


def mm(a, b):
    return lax.dot_general(a, b, (((1,), (0,)), ((), ())), preferred_element_type=F32)


def mm_nt(a, b):
    return lax.dot_general(a, b, (((1,), (1,)), ((), ())), preferred_element_type=F32)


def mm_tn(a, b):
    return lax.dot_general(a, b, (((0,), (0,)), ((), ())), preferred_element_type=F32)


def inv_rms(v):
    return lax.rsqrt(jnp.mean(v * v, axis=-1, keepdims=True) + EPS)


def rms_vjp(v, inv, g):
    return inv * g - v * (inv * inv * inv) * jnp.mean(g * v, axis=-1, keepdims=True)


def plan(ids_ref, slot_ref, n_exp, cap, blk):
    tok = ids_ref.shape[1]
    upper = (lax.broadcasted_iota(jnp.int32, (blk, blk), 0) < lax.broadcasted_iota(jnp.int32, (blk, blk), 1))
    upper = jnp.where(upper, 1.0, 0.0).astype(BF16)
    expert = lax.broadcasted_iota(jnp.int32, (n_exp, blk), 0)
    carry = jnp.zeros((n_exp, 1), F32)
    for b in range(tok // blk):
        ids = ids_ref[:, b * blk:(b + 1) * blk]
        hot = jnp.where(expert == ids, 1.0, 0.0)
        before = mm(hot.astype(BF16), upper) + carry
        rank = jnp.sum(hot * before, axis=0, keepdims=True).astype(jnp.int32)
        carry = carry + jnp.sum(hot, axis=1, keepdims=True)
        slot_ref[:, b * blk:(b + 1) * blk] = (ids & 1) * (n_exp // 2 * cap) + (ids >> 1) * cap + rank


def column(row):
    n = row.shape[1]
    return jnp.transpose(jnp.broadcast_to(row, (128, n)))[:, :1]


def dense_tile(x, w_in, w_out):
    inv = inv_rms(x)
    normed = (x * inv).astype(BF16)
    pre = mm(normed, w_in)
    hid = (pre * jax.nn.sigmoid(pre)).astype(BF16)
    h = (x + mm(hid, w_out)).astype(BF16)
    return h


def dispatch(slot_ref, rows_ref, send_ref, j, size):
    tok = slot_ref.shape[1]
    half = send_ref.shape[1]

    @pl.loop(0, half // size)
    def _(c):
        start = pl.multiple_of(c * size, size)
        want = lax.broadcasted_iota(jnp.int32, (size, tok), 0) + (start + j * half)
        pick = jnp.where(want == slot_ref[...], 1.0, 0.0).astype(BF16)
        send_ref[j, pl.ds(start, size), :] = mm(pick, rows_ref[...]).astype(BF16)


def combine(slot_row, back_ref, j):
    size = slot_row.shape[1]
    half = back_ref.shape[1]
    lane = lax.broadcasted_iota(jnp.int32, (size, half), 1) + j * half
    pick = jnp.where(lane == column(slot_row), 1.0, 0.0).astype(BF16)
    return mm(pick, back_ref[j])


ORDER = (
    14, 16, 44, 28, 25, 36, 1, 51, 10, 6, 50, 2, 9, 24, 32, 39, 18, 49, 33, 37, 48,
    12, 60, 41, 40, 8, 61, 13, 29, 62, 22, 59, 7, 20, 21, 63, 31, 45, 5, 26, 34, 47,
    46, 54, 17, 52, 58, 3, 56, 57, 35, 38, 4, 53, 55, 27, 23, 19, 11, 15, 30, 43, 42,
)


def step_kernel(cfg, *refs):
    n_pp, n_ep, side, tok, n_exp, cap, blk, chunk, eblk, pblk = cfg
    refs = list(refs)

    def take(n):
        got, refs[:] = refs[:n], refs[n:]
        return got

    ids_f, gate_f, ids_b, gate_b = take(4)
    hbm_in = take(8)
    y_out, dx_out, dwin_out, dwout_out, dwg_out, dwu_out, dwd_out = take(7)
    vm_in = take(8)
    grad, x_b, w_in, w_out, x_f, wg, wu, wd = vm_in
    in_sem, = take(1)
    slot_f, slot_b, rows_a, rows_b, h_f, h_b, y, dx = take(8)
    send_d, send_z, send_f, recv_d, recv_z, recv_f = take(6)
    send_dz, send_of, back_dz, back_of = take(4)
    dwg, dwu, dwd, acc_d = take(4)
    part, total, r1, r2, r3, turned = take(6)
    normed_b, act_b, slope_b, gz_b, gz_f = take(5)
    send_sem, recv_sem, local_sem, ar_send, ar_recv, pp_send, pp_recv, out_sem = take(8)

    me = lax.axis_index('ep')
    stage = lax.axis_index('pp')
    coord = [lax.rem(me, side), lax.rem(me // side, side), me // (side * side)]
    weight = [1, side, side * side]

    loads = [pltpu.make_async_copy(a, b, in_sem.at[i]) for i, (a, b) in enumerate(zip(hbm_in, vm_in))]
    for c in loads:
        c.start()

    barrier = pltpu.get_barrier_semaphore()

    @pl.loop(1, n_ep)
    def _(k):
        pl.semaphore_signal(barrier, inc=1, device_id={'ep': lax.rem(me + k, n_ep)}, device_id_type=MESH)

    nxt = lax.rem(stage + 1, n_pp)
    prv = lax.rem(stage + n_pp - 1, n_pp)
    pl.semaphore_signal(barrier, inc=1, device_id={'pp': nxt}, device_id_type=MESH)
    pl.semaphore_signal(barrier, inc=1, device_id={'pp': prv}, device_id_type=MESH)

    def rows_of(dev):
        return pl.ds(pl.multiple_of(dev * cap, cap), cap)

    def peer(k):
        to = 0
        for a in range(3):
            d = k // weight[a] % side
            to = to + weight[a] * lax.rem(coord[a] + lax.rem(stage * (side - d) + (1 - stage) * d, side), side)
        return to

    order = ORDER if n_ep == 64 else range(1, n_ep)

    def own(x, j, src, dst):
        return pltpu.make_async_copy(src.at[j, rows_of(me)], dst.at[j, rows_of(me)], local_sem.at[x, j])

    def start_exchange(x, j, src, dst, piece=0, pieces=1):
        if piece == 0:
            own(x, j, src, dst).start()
        n = len(order)
        for k in order[n * piece // pieces:n * (piece + 1) // pieces]:
            to = peer(k)
            pltpu.make_async_remote_copy(
                src.at[j, rows_of(to)], dst.at[j, rows_of(me)], send_sem.at[x, j], recv_sem.at[x, j],
                device_id={'ep': to}, device_id_type=MESH).start()

    def most(ref, j):
        return ref.at[j, pl.ds(0, (n_ep - 1) * cap)]

    def wait_exchange(x, j, src, dst):
        own(x, j, src, dst).wait()
        pltpu.make_async_copy(most(dst, j), most(dst, j), recv_sem.at[x, j]).wait()

    def drain_exchange(x, j, src):
        pltpu.make_async_copy(most(src, j), most(src, j), send_sem.at[x, j]).wait()

    plan(ids_b, slot_b, n_exp, cap, blk)
    loads[0].wait()

    @pl.loop(0, tok // blk)
    def _(i):
        t = pl.ds(pl.multiple_of(i * blk, blk), blk)
        rows_a[t, :] = (column(gate_b[:, t].astype(F32)) * grad[t, :].astype(F32)).astype(BF16)

    dispatch(slot_b, rows_a, send_d, 0, chunk)
    pl.semaphore_wait(barrier, n_ep + 1)
    start_exchange(0, 0, send_d, recv_d)

    for c in loads[1:]:
        c.wait()

    @pl.loop(0, tok // blk)
    def _(i):
        t = pl.ds(pl.multiple_of(i * blk, blk), blk)
        x = x_b[t, :].astype(F32)
        normed = (x * inv_rms(x)).astype(BF16)
        pre = mm(normed, w_in[...])
        sig = jax.nn.sigmoid(pre)
        act = (pre * sig).astype(BF16)
        normed_b[t, :] = normed
        act_b[t, :] = act
        slope_b[t, :] = sig * (1.0 + pre * (1.0 - sig))
        h = (x + mm(act, w_out[...])).astype(BF16)
        h_b[t, :] = h
        hf = h.astype(F32)
        rows_b[t, :] = (hf * inv_rms(hf)).astype(BF16)

    dispatch(slot_b, rows_b, send_z, 0, chunk)
    start_exchange(1, 0, send_z, recv_z)
    dispatch(slot_b, rows_a, send_d, 1, chunk)
    start_exchange(0, 1, send_d, recv_d)
    dispatch(slot_b, rows_b, send_z, 1, chunk)
    start_exchange(1, 1, send_z, recv_z)

    plan(ids_f, slot_f, n_exp, cap, blk)

    @pl.loop(0, tok // blk)
    def _(i):
        t = pl.ds(pl.multiple_of(i * blk, blk), blk)
        h = dense_tile(x_f[t, :].astype(F32), w_in[...], w_out[...])
        h_f[t, :] = h
        hf = h.astype(F32)
        rows_a[t, :] = (hf * inv_rms(hf)).astype(BF16)

    for j in range(2):
        dispatch(slot_f, rows_a, send_f, j, chunk)

    def expert_backward(e):
        dwg[e] = jnp.zeros(dwg.shape[1:], F32)
        dwu[e] = jnp.zeros(dwu.shape[1:], F32)
        acc_d[...] = jnp.zeros(acc_d.shape, F32)

        @pl.loop(0, n_ep * cap // eblk)
        def _(i):
            r = pl.ds(pl.multiple_of(i * eblk, eblk), eblk)
            x = recv_z[e, r, :]
            dy = recv_d[e, r, :]
            p = mm(x, wg[e])
            q = mm(x, wu[e])
            a = mm_nt(dy, wd[e])
            sig = jax.nn.sigmoid(p)
            act_g = p * sig
            act = (act_g * q).astype(BF16)
            dp = (a * q * (sig * (1.0 + p * (1.0 - sig)))).astype(BF16)
            dq = (a * act_g).astype(BF16)
            send_dz[e, r, :] = (mm_nt(dp, wg[e]) + mm_nt(dq, wu[e])).astype(BF16)
            dwg[e] += mm_tn(x, dp)
            dwu[e] += mm_tn(x, dq)
            acc_d[...] += mm_tn(dy, act)

        dwd[e] = jnp.transpose(acc_d[...])

    def expert_forward(e):
        @pl.loop(0, n_ep * cap // eblk)
        def _(i):
            r = pl.ds(pl.multiple_of(i * eblk, eblk), eblk)
            x = recv_f[e, r, :]
            p = mm(x, wg[e])
            q = mm(x, wu[e])
            act = (p * jax.nn.sigmoid(p) * q).astype(BF16)
            send_of[e, r, :] = mm(act, wd[e]).astype(BF16)

    for e in range(2):
        wait_exchange(0, e, send_d, recv_d)
        wait_exchange(1, e, send_z, recv_z)
        expert_backward(e)
        start_exchange(3, e, send_dz, back_dz)
        start_exchange(2, 0, send_f, recv_f, e, 2)
    start_exchange(2, 1, send_f, recv_f)
    early = [pltpu.make_async_copy(a, b, out_sem.at[i]) for i, (a, b) in enumerate(((dwg, dwg_out), (dwu, dwu_out), (dwd, dwd_out)))]
    for c in early:
        c.start()

    hid = x_b.shape[1]
    cols = part.shape[2]
    part[...] = jnp.zeros(part.shape, F32)

    def combine_half(x, j, src, back, slot, acc):
        wait_exchange(x, j, src, back)

        @pl.loop(0, tok // pblk)
        def _(i):
            t = pl.ds(pl.multiple_of(i * pblk, pblk), pblk)
            acc[t, :] = combine(slot[:, t], back, j)

    combine_half(3, 0, send_dz, back_dz, slot_b, gz_b)
    wait_exchange(3, 1, send_dz, back_dz)

    @pl.loop(0, tok // pblk)
    def _(i):
        t = pl.ds(pl.multiple_of(i * pblk, pblk), pblk)
        gz = gz_b[t, :] + combine(slot_b[:, t], back_dz, 1)
        h = h_b[t, :].astype(F32)
        dh = grad[t, :].astype(F32) + rms_vjp(h, inv_rms(h), gz)
        b = dh.astype(BF16)
        da = (mm_nt(b, w_out[...]) * slope_b[t, :]).astype(BF16)
        dwin = mm_tn(normed_b[t, :], da)
        dwout = mm_tn(b, act_b[t, :])
        for q in range(3):
            part[q, :hid, :] += dwin[:, q * cols:(q + 1) * cols]
            part[q, hid:, :] += dwout[:, q * cols:(q + 1) * cols]
        x = x_b[t, :].astype(F32)
        dx[t, :] = (dh + rms_vjp(x, inv_rms(x), mm_nt(da, w_in[...]))).astype(BF16)

    def to_stage(ref, out, i, s):
        return pltpu.make_async_remote_copy(ref, out, pp_send.at[i], pp_recv.at[i], device_id={'pp': s}, device_id_type=MESH)

    send_dx = to_stage(dx, dx_out, 0, prv)
    send_dx.start()

    rows = 2 * hid
    size = [rows // side, rows // side ** 2, rows // side ** 3]
    bufs = [r1, r2, r3]

    def base(q, depth):
        at = 0
        for j in range(depth):
            at = at + coord[(q + j) % 3] * size[j]
        return at

    def span(start, n):
        return pl.ds(pl.multiple_of(start, 8), n)

    def along(axis, d):
        c = lax.rem(coord[axis] + d, side)
        return c, me + (c - coord[axis]) * weight[axis]

    def scatter(q, j):
        axis = (q + j) % 3
        for d in range(1, side):
            c, to = along(axis, d)
            pltpu.make_async_remote_copy(
                part.at[q, span(base(q, j) + c * size[j], size[j])], bufs[j].at[q, d - 1],
                ar_send.at[j, q], ar_recv.at[j, q], device_id={'ep': to}, device_id_type=MESH).start()

    def scatter_wait(q, j):
        pltpu.make_async_copy(bufs[j].at[q], bufs[j].at[q], ar_recv.at[j, q]).wait()

    def add(q, j):
        s = span(base(q, j + 1), size[j])
        v = part[q, s, :]
        for d in range(side - 1):
            v = v + bufs[j][q, d]
        if j < 2:
            part[q, s, :] = v
        else:
            total[q, s, :] = v

    def gather(q, j):
        axis = (q + j) % 3
        s = span(base(q, j + 1), size[j])
        for d in range(1, side):
            c, to = along(axis, d)
            pltpu.make_async_remote_copy(
                total.at[q, s], total.at[q, s], ar_send.at[3 + j, q], ar_recv.at[3 + j, q],
                device_id={'ep': to}, device_id_type=MESH).start()

    def gather_wait(q, j):
        n = (side - 1) * size[j]
        pltpu.make_async_copy(total.at[q, pl.ds(0, n)], total.at[q, pl.ds(0, n)], ar_recv.at[3 + j, q]).wait()

    for q in range(3):
        scatter(q, 0)
    wait_exchange(2, 0, send_f, recv_f)
    expert_forward(0)
    start_exchange(4, 0, send_of, back_of, 0, 2)
    wait_exchange(2, 1, send_f, recv_f)
    expert_forward(1)
    for j in range(3):
        for q in range(3):
            scatter_wait(q, j)
            add(q, j)
            if j < 2:
                scatter(q, j + 1)
            else:
                gather(q, 2)
        start_exchange(4, (j + 1) // 2, send_of, back_of, (j + 1) % 2, 2)
    for j in (2, 1):
        for q in range(3):
            gather_wait(q, j)
            gather(q, j - 1)

    combine_half(4, 0, send_of, back_of, slot_f, gz_f)
    wait_exchange(4, 1, send_of, back_of)

    @pl.loop(0, tok // pblk)
    def _(i):
        t = pl.ds(pl.multiple_of(i * pblk, pblk), pblk)
        picked = gz_f[t, :] + combine(slot_f[:, t], back_of, 1)
        y[t, :] = (h_f[t, :].astype(F32) + picked * column(gate_f[:, t].astype(F32))).astype(BF16)

    send_y = to_stage(y, y_out, 1, nxt)
    send_y.start()

    late = []
    for q in range(3):
        gather_wait(q, 0)
        late.append(pltpu.make_async_copy(total.at[q, pl.ds(0, hid)], dwin_out.at[:, pl.ds(q * cols, cols)], out_sem.at[3 + q]))
        late[-1].start()
        turned[q * cols:(q + 1) * cols, :] = jnp.transpose(total[q, hid:, :])
    late.append(pltpu.make_async_copy(turned, dwout_out, out_sem.at[6]))
    late[-1].start()

    for x, src in enumerate((send_d, send_z, send_f, send_dz, send_of)):
        for j in range(2):
            drain_exchange(x, j, src)
    for j in range(3):
        for q in range(3):
            n = pl.ds(0, (side - 1) * size[j])
            pltpu.make_async_copy(total.at[q, n], total.at[q, n], ar_send.at[j, q]).wait()
            pltpu.make_async_copy(total.at[q, n], total.at[q, n], ar_send.at[3 + j, q]).wait()
    for c in early + late:
        c.wait()
    send_dx.wait()
    send_y.wait()


def write_kernel(n, *refs):
    ins, outs, hold, sem = refs[:n], refs[n:2 * n], refs[2 * n:3 * n], refs[3 * n]
    gets = [pltpu.make_async_copy(ins[i], hold[i], sem.at[0, i]) for i in range(n)]
    puts = [pltpu.make_async_copy(hold[i], outs[i], sem.at[1, i]) for i in range(n)]
    for c in gets:
        c.start()
    for get, put in zip(gets, puts):
        get.wait()
        put.start()
    for c in puts:
        c.wait()


def write(*arrays):
    n = len(arrays)
    shapes = [jax.ShapeDtypeStruct(a.shape, a.dtype) for a in arrays]
    return pl.pallas_call(
        functools.partial(write_kernel, n), out_shape=shapes, in_specs=[ANY] * n, out_specs=[ANY] * n,
        scratch_shapes=[pltpu.VMEM(a.shape, a.dtype) for a in arrays] + [pltpu.SemaphoreType.DMA((2, n))],
        compiler_params=pltpu.CompilerParams(vmem_limit_bytes=62 * MIB),
    )(*arrays)


def solution(mesh):
    n_ep = mesh.shape['ep']
    n_pp = mesh.shape['pp']
    side = round(n_ep ** (1 / 3))
    tok_spec = P('pp', 'ep', None)
    dense_spec = P('pp', None, None)
    exp_spec = P('pp', 'ep', None, None)

    def body(x_fwd, ids_fwd, gates_fwd, x_saved, grad_out, ids_bwd, gates_bwd, w_in, w_out, w_gate, w_up, w_down):
        x_fwd, x_saved, grad_out = x_fwd[0], x_saved[0], grad_out[0]
        w_in, w_out, w_gate, w_up, w_down = w_in[0], w_out[0], w_gate[0], w_up[0], w_down[0]
        tok, hid = x_fwd.shape
        ff = w_in.shape[1]
        n_exp = w_gate.shape[0] * n_ep
        eff = w_gate.shape[2]
        cap = 2 * tok // n_exp
        blk = min(256, tok)
        chunk = min(512, n_ep * cap)
        eblk = min(512, n_ep * cap)
        pblk = min(512, tok)
        cfg = (n_pp, n_ep, side, tok, n_exp, cap, blk, chunk, eblk, pblk)
        ids_f, ids_b = ids_fwd.reshape(1, tok), ids_bwd.reshape(1, tok)
        gate_f, gate_b = gates_fwd.reshape(1, tok), gates_bwd.reshape(1, tok)
        big = [grad_out, x_saved, w_in, w_out, x_fwd, w_gate, w_up, w_down]
        slots = pltpu.VMEM((2, n_ep * cap, hid), BF16)
        rows = pltpu.VMEM((tok, hid), BF16)
        route = pltpu.VMEM((1, tok), jnp.int32)
        dma = pltpu.SemaphoreType.DMA
        cols = ff // 3
        outs = [((tok, hid), BF16)] * 2 + [(w.shape, F32) for w in (w_in, w_out, w_gate, w_up, w_down)]
        results = pl.pallas_call(
            functools.partial(step_kernel, cfg),
            out_shape=[jax.ShapeDtypeStruct(*o) for o in outs],
            in_specs=[VMEM] * 4 + [ANY] * 8,
            out_specs=[ANY] * 7,
            scratch_shapes=[pltpu.VMEM(b.shape, b.dtype) for b in big] + [dma((8,))]
            + [route] * 2 + [rows] * 6 + [slots] * 10
            + [pltpu.VMEM(w.shape, F32) for w in (w_gate, w_up, w_down)] + [pltpu.VMEM((hid, eff), F32)]
            + [pltpu.VMEM((3, 2 * hid, cols), F32)] * 2
            + [pltpu.VMEM((3, side - 1, 2 * hid // side ** j, cols), F32) for j in (1, 2, 3)]
            + [pltpu.VMEM((ff, hid), F32)]
            + [rows, pltpu.VMEM((tok, ff), BF16), pltpu.VMEM((tok, ff), F32), pltpu.VMEM((tok, hid), F32), pltpu.VMEM((tok, hid), F32)]
            + [dma((5, 2)), dma((5, 2)), dma((5, 2)), dma((6, 3)), dma((6, 3)), dma((2,)), dma((2,)), dma((7,))],
            compiler_params=pltpu.CompilerParams(collective_id=0, has_side_effects=True, vmem_limit_bytes=63 * MIB),
        )(ids_f, gate_f, ids_b, gate_b, *big)
        y_next, dx_prev, dw_in, dw_out, dw_gate, dw_up, dw_down = write(*results)
        return (y_next[None], dx_prev[None], dw_in[None], dw_out[None], dw_gate[None], dw_up[None], dw_down[None])

    return jax.shard_map(body, mesh=mesh,
                         in_specs=(tok_spec, tok_spec, tok_spec, tok_spec, tok_spec, tok_spec, tok_spec, dense_spec, dense_spec, exp_spec, exp_spec, exp_spec),
                         out_specs=(tok_spec, tok_spec, dense_spec, dense_spec, exp_spec, exp_spec, exp_spec),
                         check_vma=False)
```
